256 devices in a mesh: dp: 32 (over x, z), tensor: 8 (over y, core).
Axes of the slice: x: 4, y: 4, z: 8, core: 2. Of those that a mesh axis runs over, the one named last changes fastest.
Arguments:
- vis_rows: bfloat16 [8, 256, 2, 3200], P(None, 'dp', None, 'tensor'), may hold values from -6 to 6
- ln_gain: float32 [2, 3200], replicated, may hold values from 0.25 to 1.75
- ln_bias: float32 [2, 3200], replicated, may hold values from -3 to 3
- proj_weight: bfloat16 [3200, 2, 8192], P('dp', None, 'tensor'), may hold values from -0.078125 to 0.078125
- text_rows: bfloat16 [32, 384, 8192], P('dp', None, 'tensor'), may hold values from -8 to 8
- attn_gain: float32 [8192], replicated, may hold values from 0.25 to 1.75
- w_query: bfloat16 [8192, 4096], P('dp', 'tensor'), may hold values from -0.088388348 to 0.088388348
- key_value_weight: bfloat16 [8192, 2, 1024], P('dp', None, 'tensor'), may hold values from -0.088388348 to 0.088388348
- tile_counts: int32 [32], replicated, may hold values from 1 to 16, 256 in all
- image_offsets: int32 [32], P('dp'), may hold values from 0 to 256
Outputs:
- attn_context: bfloat16 [32, 384, 4096], P('dp', None, 'tensor')
The draws below stay inside these ranges and needn't reach their ends.
Inputs may be any that keep to these rules, and one draw needn't show every extreme that they name: tile_counts counts all 256 tiles, and its largest entry is exactly 16.
All inputs are finite; a program needn't handle non-finite values.
Results may differ from the reference program's by a relative error of at most 0.0074.
Values may be sent and summed in bfloat16 or wider, within the bound.
No kernel may reach another device: no remote copies, remote signals or barrier semaphores. Data moves between devices by JAX's collectives and lax.ppermute only.
A program may use at most 128 MiB of HBM per device.

```python
import math
import jax
import jax.numpy as jnp
import numpy as np
from jax import lax

DV = 3200
MERGE = 2
PW = 6400
MODEL_WIDTH = 8192
QUERY_HEADS = 32
KEY_VALUE_HEADS = 8
HEAD_WIDTH = 128
TILE_DEV = 8
TILE_TOK = 8
SEQUENCE_LENGTH = 384
SAMPLES = 32
TILES = 256
ROW_TOK = 256
MAXT_TILES = 16
N_DP = 32


def draw_w_query(key, part):
    bound_value = 8.0 * MODEL_WIDTH ** (-0.5)
    sampled_values = jnp.clip(jax.random.normal(jax.random.fold_in(key, 1), (MODEL_WIDTH, QUERY_HEADS * HEAD_WIDTH), jnp.float32), -4.0, 4.0) * MODEL_WIDTH ** (-0.5)
    return jnp.clip(sampled_values, -bound_value, bound_value).astype(jnp.bfloat16)


def draw_key_value_weight(key, part):
    bound_value = 8.0 * MODEL_WIDTH ** (-0.5)
    sampled_values = jnp.clip(jax.random.normal(jax.random.fold_in(key, 2), (MODEL_WIDTH, 2, KEY_VALUE_HEADS * HEAD_WIDTH), jnp.float32), -4.0, 4.0) * MODEL_WIDTH ** (-0.5)
    return jnp.clip(sampled_values, -bound_value, bound_value).astype(jnp.bfloat16)


def draw_text_rows(key, part):
    sampled_values = jnp.clip(jax.random.normal(jax.random.fold_in(key, 3), (SAMPLES, SEQUENCE_LENGTH, MODEL_WIDTH), jnp.float32), -5.0, 5.0)
    return jnp.clip(sampled_values, -8.0, 8.0).astype(jnp.bfloat16)


def with_ends(entries, own_key, smallest, top_value):
    index_at = [jax.random.randint(jax.random.fold_in(own_key, axis), (), 0, length) for axis, length in enumerate(entries.shape)]
    widest = entries.shape.index(max(entries.shape))
    beside = index_at[:widest] + [(index_at[widest] + 1) % entries.shape[widest]] + index_at[widest + 1:]
    return entries.at[tuple(index_at)].set(smallest).at[tuple(beside)].set(top_value)


def shard_levels(key, dims, pieces, smallest, largest):
    def one(axis_at, shards_of):
        draws = jax.random.uniform(jax.random.fold_in(jax.random.fold_in(key, 6), axis_at), (shards_of,), jnp.float32, smallest / len(pieces), largest / len(pieces))
        return jnp.repeat(jnp.exp(draws), dims[axis_at] // shards_of).reshape((-1,) + (1,) * (len(dims) - axis_at - 1))

    level = one(*pieces[0])
    for cut in pieces[1:]:
        level = level * one(*cut)
    return level


def profile(number_of, total, most, lean):
    loads = [(1 << 20) // math.isqrt(rank ** lean) + 1 for rank in range(2, number_of + 1)]
    spare, given = total - most - (number_of - 1), [1] * (number_of - 1)
    while spare > 0:
        movable = [i for i in range(number_of - 1) if given[i] < most]
        pool, left = sum([loads[i] for i in movable]), spare
        for i in movable:
            extra = min(most - given[i], max(1, left * loads[i] // pool), spare)
            given[i] = given[i] + extra
            spare = spare - extra
    return np.array([most] + given)


def uneven_parts(stream_key, number_of, total, most, slope):
    if number_of == 2:
        one = jax.random.randint(stream_key, (), max(1, total - most), min(most, total - 1) + 1)
        return jnp.stack([one, total - one])
    lengths = jnp.asarray(profile(number_of, total, most, slope), jnp.int32)
    couples = (number_of - 1) // 2
    source_of, receiver = lengths[1:1 + 2 * couples:2], lengths[2:2 + 2 * couples:2]
    room = jnp.minimum(source_of - 1, most - receiver)
    moved = jax.random.randint(jax.random.fold_in(stream_key, 1), (couples,), 0, 1 << 20) % (room + 1)
    lengths = lengths.at[1:1 + 2 * couples:2].set(source_of - moved).at[2:2 + 2 * couples:2].set(receiver + moved)
    return lengths[jax.random.permutation(jax.random.fold_in(stream_key, 2), number_of)]


def normal_values(own_key, dims, scale, bound, split=(), kind=jnp.bfloat16):
    level = shard_levels(own_key, dims, split, -0.22, 0.18) if split else 1.0
    entries = jax.random.normal(own_key, dims, jnp.float32) * scale * level
    return jnp.minimum(jnp.maximum(entries, -bound), bound).astype(kind)


def setup_inputs(seed: int = 0) -> dict:
    key_of = jax.random.split(jax.random.key(seed), 11)
    return {
        "vis_rows": normal_values(key_of[0], (TILE_DEV, ROW_TOK, MERGE, DV), 1.0, 6.0, ((1, 32), (3, 8))),
        "ln_gain": jnp.clip(1.0 + 0.15 * jax.random.normal(key_of[1], (MERGE, DV), jnp.float32), 0.25, 1.75),
        "ln_bias": normal_values(key_of[2], (MERGE, DV), 0.5, 3.0, (), jnp.float32),
        "proj_weight": normal_values(key_of[3], (DV, MERGE, MODEL_WIDTH), PW ** -0.5, 0.078125, ((0, 32), (2, 8))),
        "text_rows": draw_text_rows(jax.random.fold_in(key_of[10], 71), 0),
        "attn_gain": jnp.clip(1.0 + 0.15 * jax.random.normal(key_of[5], (MODEL_WIDTH,), jnp.float32), 0.25, 1.75),
        "w_query": draw_w_query(jax.random.fold_in(key_of[10], 71), 0),
        "key_value_weight": draw_key_value_weight(jax.random.fold_in(key_of[10], 71), 0),
        "tile_counts": uneven_parts(key_of[8], SAMPLES, TILES, MAXT_TILES, 2).astype(jnp.int32),
        "image_offsets": with_ends(jax.random.randint(key_of[9], (SAMPLES,), 0, SEQUENCE_LENGTH - MAXT_TILES * TILE_TOK + 1), jax.random.fold_in(key_of[9], 1), 0, SEQUENCE_LENGTH - MAXT_TILES * TILE_TOK).astype(jnp.int32),
    }


vision_epsilon = 1e-06
decoder_epsilon = 1e-05
rope_base = 500000.0

def apply_rotary(value_rows, position_indices):
    half_width = value_rows.shape[-1] // 2
    exponents = jnp.arange(half_width, dtype=jnp.float32) * (2.0 / value_rows.shape[-1])
    frequency = rope_base ** (-exponents)
    angles = position_indices.astype(jnp.float32)[:, None] * frequency[None, :]
    cosine = jnp.cos(angles)[:, None, :]
    sine = jnp.sin(angles)[:, None, :]
    first_half = value_rows[..., :half_width]
    second_half = value_rows[..., half_width:]
    return jnp.concatenate([first_half * cosine - second_half * sine, second_half * cosine + first_half * sine], axis=-1)

def layer_norm(value_rows, gain, bias_values):
    average = lax.optimization_barrier(jnp.mean(value_rows, axis=(-2, -1), keepdims=True))
    centered = value_rows - average
    variance = lax.optimization_barrier(jnp.mean(centered * centered, axis=(-2, -1), keepdims=True))
    return centered * lax.rsqrt(variance + vision_epsilon) * gain + bias_values

def decoder_sample(sequence, w_query, key_value_weight, attn_gain):
    seq_float = sequence.astype(jnp.float32)
    mean_square = lax.optimization_barrier(jnp.mean(seq_float * seq_float, axis=-1, keepdims=True))
    normalized_sequence = (seq_float * lax.rsqrt(mean_square + decoder_epsilon) * attn_gain).astype(jnp.bfloat16)
    query_full = jnp.dot(normalized_sequence, w_query, preferred_element_type=jnp.float32)
    key_value_complete = jnp.dot(normalized_sequence, key_value_weight.reshape(MODEL_WIDTH, 2 * KEY_VALUE_HEADS * HEAD_WIDTH), preferred_element_type=jnp.float32)
    key_value_complete = key_value_complete.reshape(SEQUENCE_LENGTH, 2, KEY_VALUE_HEADS * HEAD_WIDTH)
    position_indices = jnp.arange(SEQUENCE_LENGTH, dtype=jnp.int32)
    query_group_count = QUERY_HEADS // KEY_VALUE_HEADS
    query_rows = apply_rotary(query_full.reshape(SEQUENCE_LENGTH, QUERY_HEADS, HEAD_WIDTH), position_indices).astype(jnp.bfloat16)
    query_rows = query_rows.reshape(SEQUENCE_LENGTH, KEY_VALUE_HEADS, query_group_count, HEAD_WIDTH)
    key_rows = apply_rotary(key_value_complete[:, 0].reshape(SEQUENCE_LENGTH, KEY_VALUE_HEADS, HEAD_WIDTH), position_indices).astype(jnp.bfloat16)
    value_rows = key_value_complete[:, 1].reshape(SEQUENCE_LENGTH, KEY_VALUE_HEADS, HEAD_WIDTH).astype(jnp.bfloat16)
    scores = jnp.einsum('pgjd,kgd->gjpk', query_rows.astype(jnp.float32), key_rows.astype(jnp.float32)) * HEAD_WIDTH ** (-0.5)
    causal = position_indices[:, None] >= position_indices[None, :]
    scores = jnp.where(causal[None, None], scores, -1e+30)
    row_max = lax.optimization_barrier(jnp.max(scores, axis=-1, keepdims=True))
    exponentials = jnp.exp(scores - row_max)
    weights = (exponentials / lax.optimization_barrier(jnp.sum(exponentials, axis=-1, keepdims=True))).astype(jnp.bfloat16)
    context = jnp.einsum('gjpk,kgd->pgjd', weights.astype(jnp.float32), value_rows.astype(jnp.float32))
    return context.astype(jnp.bfloat16).reshape(SEQUENCE_LENGTH, QUERY_HEADS * HEAD_WIDTH)

def reference(vis_rows, ln_gain, ln_bias, proj_weight, text_rows, attn_gain, w_query, key_value_weight, tile_counts, image_offsets):
    merged = vis_rows.reshape(TILE_DEV * ROW_TOK, MERGE, DV).astype(jnp.float32)
    normed_vis = layer_norm(merged, ln_gain, ln_bias).astype(jnp.bfloat16)
    flat_weight = jnp.transpose(proj_weight, (1, 0, 2)).reshape(MERGE * DV, MODEL_WIDTH)
    image_cols = jnp.dot(normed_vis.reshape(TILE_DEV * ROW_TOK, MERGE * DV), flat_weight, preferred_element_type=jnp.float32).astype(jnp.bfloat16)
    image_tiles = image_cols.reshape(TILE_DEV, N_DP, TILE_TOK, MODEL_WIDTH).reshape(TILES, TILE_TOK, MODEL_WIDTH)
    tile_ends = jnp.cumsum(tile_counts).astype(jnp.int32)
    tile_first = (tile_ends - tile_counts).astype(jnp.int32)
    tile_order = jnp.arange(MAXT_TILES, dtype=jnp.int32)
    image_span = MAXT_TILES * TILE_TOK

    def per_sample(inputs):
        sequence, first_tile, count, offset = inputs
        picked = jnp.clip(first_tile + tile_order, 0, TILES - 1).astype(jnp.int32)
        arrived = image_tiles[picked].reshape(image_span, MODEL_WIDTH)
        start_row = offset.astype(jnp.int32)
        current = lax.dynamic_slice_in_dim(sequence, start_row, image_span, 0)
        is_image = jnp.repeat(tile_order < count, TILE_TOK)[:, None]
        merged_rows = jnp.where(is_image, arrived, current)
        sequence = lax.dynamic_update_slice_in_dim(sequence, merged_rows, start_row, 0)
        return decoder_sample(sequence, w_query, key_value_weight, attn_gain)
    return lax.map(per_sample, (text_rows, tile_first, tile_counts, image_offsets))
```

```python
import jax
import jax.numpy as jnp
from jax import lax
from jax.experimental import pallas as pl
from jax.experimental.pallas import tpu as pltpu
from jax.sharding import Mesh, PartitionSpec as P

HEAD = 128
NX, NZ, NY, NC = 4, 8, 4, 2
SEQ = 384
SPAN = 128
WIDTH = 8192
vision_epsilon = 1e-06
decoder_epsilon = 1e-05
rope_base = 500000.0


def shift(array, axis, by):
    size = lax.axis_size(axis)
    return lax.ppermute(array, axis, [(i, (i + by) % size) for i in range(size)])


def ring4(array, axis):
    rows = array.shape[0]
    half = rows // 2
    below = shift(array, axis, 1)
    above = shift(array, axis, -1)
    far_low = shift(below[:half], axis, 1)
    far_high = shift(above[half:], axis, -1)
    return [(array, 0, 0), (below, -1, 0), (above, 1, 0), (far_low, 2, 0), (far_high, 2, half)]


def ring8(array, axis):
    rows = array.shape[0]
    half = rows // 2
    pieces = [(array, 0, 0)]
    below = above = array
    for step in (1, 2, 3):
        below = shift(below, axis, 1)
        above = shift(above, axis, -1)
        pieces += [(below, -step, 0), (above, step, 0)]
    pieces += [
        (shift(below[:half], axis, 1), 4, 0),
        (shift(above[half:], axis, -1), 4, half),
    ]
    return pieces


def gather_features(array):
    pieces = [(a, dy, 0, r) for a, dy, r in ring4(array, "y")]
    return pieces + [(shift(a, "c", 1), dy, 1, r) for a, dy, _, r in pieces]


def rope_tables():
    half = HEAD // 2
    exponents = jnp.arange(half, dtype=jnp.float32) * (2.0 / HEAD)
    frequency = rope_base ** (-exponents)
    positions = jnp.arange(SEQ, dtype=jnp.int32).astype(jnp.float32)
    angles = positions[:, None] * frequency[None, :]
    cosine, sine = jnp.cos(angles), jnp.sin(angles)
    return (
        jnp.concatenate([cosine, cosine], axis=1),
        jnp.concatenate([-sine, sine], axis=1),
    )


def decoder(where, text, image, query_w, keyval_w, gain, cosine, sine):
    arrays, plan = [], []
    for group, name in ((text, "t"), (image, "i")):
        for a, dy, flip, row in group:
            plan.append((name, len(arrays), dy, flip, row, a.shape[0]))
            arrays.append(a)
    weights = []
    for group, col, cols in ((query_w, 0, 512), (keyval_w, 512, 256)):
        for a, parts in group:
            for dx, dz, row, rows, at in parts:
                weights.append((len(arrays), dx, dz, row, rows, at, col, cols))
            arrays.append(a)
    count = len(arrays)
    n_act, n_w = len(plan), len(weights)

    def kernel(where_ref, *refs):
        srcs = refs[:count]
        gain_ref, cos_ref, sin_ref = refs[count : count + 3]
        out_ref = refs[count + 3]
        a_ref, i_ref, b_ref, q_ref, act_sem, w_sem = refs[count + 4 :]
        x, z, y, c = where_ref[0], where_ref[1], where_ref[2], where_ref[3]
        start, n_rows = where_ref[4], where_ref[5]

        acts = []
        for k, (name, n, dy, flip, row, rows) in enumerate(plan):
            core = c if flip == 0 else 1 - c
            t = lax.rem(y + (dy + NY), NY) * NC + core
            target = (a_ref if name == "t" else i_ref).at[t, pl.ds(row, rows), :]
            acts.append(pltpu.make_async_copy(srcs[n], target, act_sem.at[k]))
        for copy in acts:
            copy.start()
        loads = []
        for k, (n, dx, dz, row, rows, at, col, cols) in enumerate(weights):
            d = lax.rem(x + (dx + NX), NX) * NZ + lax.rem(z + (dz + NZ), NZ)
            first = pl.multiple_of(d * 256 + row, 64)
            loads.append(
                pltpu.make_async_copy(
                    srcs[n].at[pl.ds(at, rows), :],
                    b_ref.at[pl.ds(first, rows), pl.ds(col, cols)],
                    w_sem.at[k],
                )
            )
        for copy in loads:
            copy.start()
        for copy in acts:
            copy.wait()
        p_at = lax.broadcasted_iota(jnp.int32, (SEQ, SPAN), 0) - start
        j_at = lax.broadcasted_iota(jnp.int32, (SEQ, SPAN), 1)
        pick = jnp.where((p_at == j_at) & (j_at < n_rows), 1.0, 0.0).astype(jnp.bfloat16)
        rows_at = lax.broadcasted_iota(jnp.int32, (SEQ, 1), 0) - start
        is_image = (rows_at >= 0) & (rows_at < n_rows)

        def insert(t, total):
            placed = jnp.dot(pick, i_ref[t], preferred_element_type=jnp.float32)
            value = jnp.where(is_image, placed, a_ref[t].astype(jnp.float32))
            a_ref[t] = value.astype(jnp.bfloat16)
            return total + jnp.sum(value * value, axis=1, keepdims=True)

        total = lax.fori_loop(0, 8, insert, jnp.zeros((SEQ, 1), jnp.float32))
        scale = lax.rsqrt(total * (1.0 / WIDTH) + decoder_epsilon)

        def normalize(t, carry):
            a_ref[t] = (
                a_ref[t].astype(jnp.float32) * scale * gain_ref[pl.ds(t, 1), :]
            ).astype(jnp.bfloat16)
            return carry

        lax.fori_loop(0, 8, normalize, 0)
        for copy in loads:
            copy.wait()
        q_ref[...] = jnp.zeros(q_ref.shape, jnp.float32)

        def project(t, carry):
            q_ref[...] += jnp.dot(
                a_ref[t], b_ref[pl.ds(t * 1024, 1024), :], preferred_element_type=jnp.float32
            )
            return carry

        lax.fori_loop(0, 8, project, 0)
        cos, sin = cos_ref[...], sin_ref[...]

        def rotated(value):
            return (value * cos + pltpu.roll(value, 64, 1) * sin).astype(jnp.bfloat16)

        key = rotated(q_ref[:, 512:640])
        value = q_ref[:, 640:768].astype(jnp.bfloat16)
        causal = lax.broadcasted_iota(jnp.int32, (SEQ, SEQ), 0) >= lax.broadcasted_iota(
            jnp.int32, (SEQ, SEQ), 1
        )
        for h in range(4):
            query = rotated(q_ref[:, h * HEAD : (h + 1) * HEAD])
            scores = lax.dot_general(
                query, key, (((1,), (1,)), ((), ())), preferred_element_type=jnp.float32
            ) * (HEAD ** (-0.5))
            scores = jnp.where(causal, scores, -1e30)
            top = jnp.max(scores, axis=1, keepdims=True)
            e = jnp.exp(scores - top)
            w = (e / jnp.sum(e, axis=1, keepdims=True)).astype(jnp.bfloat16)
            out_ref[:, h * HEAD : (h + 1) * HEAD] = jnp.dot(
                w, value, preferred_element_type=jnp.float32
            ).astype(jnp.bfloat16)

    any_spec = pl.BlockSpec(memory_space=pl.ANY)
    vmem = pl.BlockSpec(memory_space=pltpu.VMEM)
    return pl.pallas_call(
        kernel,
        out_shape=jax.ShapeDtypeStruct((SEQ, 512), jnp.bfloat16),
        in_specs=[pl.BlockSpec(memory_space=pltpu.SMEM)] + [any_spec] * count + [vmem] * 3,
        out_specs=vmem,
        scratch_shapes=[
            pltpu.VMEM((8, SEQ, 1024), jnp.bfloat16),
            pltpu.VMEM((8, SPAN, 1024), jnp.bfloat16),
            pltpu.VMEM((WIDTH, 768), jnp.bfloat16),
            pltpu.VMEM((SEQ, 768), jnp.float32),
            pltpu.SemaphoreType.DMA((n_act,)),
            pltpu.SemaphoreType.DMA((n_w,)),
        ],
        compiler_params=pltpu.CompilerParams(vmem_limit_bytes=48 * 1024 * 1024),
        name="decoder",
    )(where, *arrays, gain, cosine, sine)


def vision(vis_rows, ln_gain, ln_bias, proj_weight, x, z, y, c):
    tokens = vis_rows.shape[0] * vis_rows.shape[1]
    own_w = jnp.swapaxes(proj_weight, 0, 1).reshape(200, 1024)
    below_w = shift(own_w, "x", 1)
    above_w = shift(own_w, "x", -1)
    far_low = shift(below_w[:96], "x", 1)
    far_high = shift(above_w[96:], "x", -1)
    part = vis_rows.reshape(tokens, 2, 400).astype(jnp.float32)
    mean = jnp.mean(part, axis=(1, 2))
    dev = jnp.sum(jnp.square(part - mean[:, None, None]), axis=(1, 2))
    stats = jnp.stack([mean, dev])
    other = shift(stats, "c", 1)
    mean2 = (stats[0] + other[0]) * 0.5
    dev2 = stats[1] + other[1] + 400.0 * jnp.square(stats[0] - other[0])
    stats = jnp.stack([mean2, dev2])
    all_stats = jnp.stack([stats, shift(stats, "y", 1), shift(stats, "y", -1), shift(stats, "y", 2)])
    mean = jnp.mean(all_stats[:, 0], axis=0)
    variance = (
        jnp.sum(all_stats[:, 1], axis=0)
        + 1600.0 * jnp.sum(jnp.square(all_stats[:, 0] - mean[None]), axis=0)
    ) * (1.0 / 6400.0)
    t = y * NC + c
    gain = lax.dynamic_slice_in_dim(ln_gain, t * 400, 400, 1)
    bias = lax.dynamic_slice_in_dim(ln_bias, t * 400, 400, 1)
    normed = (
        (part - mean[:, None, None]) * lax.rsqrt(variance + vision_epsilon)[:, None, None] * gain
        + bias
    ).astype(jnp.bfloat16)
    blocks = jnp.moveaxis(normed.reshape(tokens, 2, 4, 100), 2, 0).reshape(4, tokens, 200)
    rounds = []
    for r in range(4):
        block = lax.dynamic_index_in_dim(blocks, lax.rem(z + r, 4), 0, keepdims=False)
        pairs = [
            (zz * NC + cc, (4 * cc + (zz % 4 + r) % 4) * NC + zz // 4)
            for zz in range(NZ)
            for cc in range(NC)
        ]
        rounds.append(lax.ppermute(block, ("z", "c"), pairs))
    mine = jnp.stack(rounds)
    by_y = jnp.stack([mine, shift(mine, "y", -1), shift(mine, "y", 2), shift(mine, "y", 1)])
    by_y_other = shift(by_y, "c", 1)
    low = jnp.where(c == 0, by_y, by_y_other)
    high = jnp.where(c == 0, by_y_other, by_y)
    acts = jnp.stack([low, high], axis=1).reshape(4, 8 * tokens, 200)
    far_w = jnp.concatenate([far_low, far_high], axis=0)
    partial = None
    for dx, w in ((0, own_w), (-1, below_w), (1, above_w), (2, far_w)):
        a = lax.dynamic_index_in_dim(acts, lax.rem(x + dx - y + 8, 4), 0, keepdims=False)
        term = jnp.dot(a, w, preferred_element_type=jnp.float32)
        partial = term if partial is None else partial + term
    partial = partial.astype(jnp.bfloat16).reshape(8, tokens, 1024)

    def set_for(delta):
        target = lax.rem(z + delta, 8)
        index = (target // 4) * 4 + (-delta) % 4
        return lax.dynamic_index_in_dim(partial, index, 0, keepdims=False)

    total = set_for(0).astype(jnp.float32)
    arrived = [shift(set_for(delta), "z", delta) for delta in range(1, 8)]
    for a in arrived:
        total = total + a.astype(jnp.float32)
    return total.astype(jnp.bfloat16).reshape(8, 8, 1024)


def per_device(
    vis_rows, ln_gain, ln_bias, proj_weight, text_rows, attn_gain, w_query,
    key_value_weight, tile_counts, image_offsets,
):
    x, z = lax.axis_index("x"), lax.axis_index("z")
    y, c = lax.axis_index("y"), lax.axis_index("c")
    dp = x * NZ + z
    tile_ends = jnp.cumsum(tile_counts)
    tile_firsts = tile_ends - tile_counts
    sample_ids = jnp.arange(32, dtype=jnp.int32)
    tiles_here = jnp.arange(8, dtype=jnp.int32) * 32 + dp
    owners = jnp.sum((tile_ends[None, :] <= tiles_here[:, None]).astype(jnp.int32), axis=1)
    is_mine = sample_ids == dp
    my_first = jnp.sum(jnp.where(is_mine, tile_firsts, 0))
    my_count = jnp.sum(jnp.where(is_mine, tile_counts, 0))

    image = vision(vis_rows, ln_gain, ln_bias, proj_weight, x, z, y, c)

    text = gather_features(text_rows[0])

    keyval = key_value_weight.reshape(256, 256)
    along_x = ring4(keyval, "x")
    order = (0, -1, 1, 2)
    stack = jnp.concatenate([a for a, _, _ in along_x], axis=0)
    keyval_w = []
    for a, dz, row in ring8(stack, "z"):
        parts = [
            (order[n], dz, 0, 256, n * 256 - row)
            for n in range(4)
            if row <= n * 256 and n * 256 + 256 <= row + a.shape[0]
        ]
        keyval_w.append((a, parts))

    query_w = []
    for piece, dz, row in ring8(w_query, "z"):
        for a, dx, more in ring4(piece, "x"):
            query_w.append((a, [(dx, dz, row + more, a.shape[0], 0)]))

    slots = jnp.zeros((32, 8, 1024), jnp.bfloat16)
    for r in range(8):
        slots = jnp.where((owners[r] == sample_ids)[:, None, None], image[r][None], slots)
    received = lax.all_to_all(slots, ("x", "z"), split_axis=0, concat_axis=0, tiled=True)
    sources = (my_first + jnp.arange(16, dtype=jnp.int32)) % 32
    mine = received[sources].reshape(SPAN, 1024)
    image_all = gather_features(mine)

    where = jnp.stack([x, z, y, c, image_offsets[0], my_count * 8]).astype(jnp.int32)
    cosine, sine = rope_tables()
    out = decoder(
        where, text, image_all, query_w, keyval_w, attn_gain.reshape(8, 1024), cosine, sine
    )
    return out[None]


def solution(mesh):
    fine = Mesh(mesh.devices.reshape(NX, NZ, NY, NC), ("x", "z", "y", "c"))
    dp, tensor = ("x", "z"), ("y", "c")
    in_specs = (
        P(None, dp, None, tensor), P(), P(), P(dp, None, tensor), P(dp, None, tensor), P(),
        P(dp, tensor), P(dp, None, tensor), P(), P(dp),
    )
    return jax.shard_map(
        per_device, mesh=fine, in_specs=in_specs, out_specs=P(dp, None, tensor), check_vma=False
    )
```

```python
import jax
import jax.numpy as jnp
from jax import lax
from jax.experimental import pallas as pl
from jax.experimental.pallas import tpu as pltpu
from jax.sharding import Mesh, PartitionSpec as P


HEAD = 128
NX, NZ, NY, NC = 4, 8, 4, 2
SEQ = 384
SPAN = 128
WIDTH = 8192
vision_epsilon = 1e-06
decoder_epsilon = 1e-05
rope_base = 500000.0


def shift(array, axis, by):
    size = lax.axis_size(axis)
    return lax.ppermute(array, axis, [(i, (i + by) % size) for i in range(size)])


def exchange(array, axis):
    return lax.all_to_all(array, axis, 0, 0, tiled=True)


def ring4(array, axis):
    half = array.shape[0] // 2
    below = shift(array, axis, 1)
    above = shift(array, axis, -1)
    far_low = shift(below[:half], axis, 1)
    far_high = shift(above[half:], axis, -1)
    return [(array, 0, 0), (below, -1, 0), (above, 1, 0), (far_low, 2, 0), (far_high, 2, half)]


def ring8(array, axis):
    half = array.shape[0] // 2
    pieces = [(array, 0, 0)]
    below = above = array
    for step in (1, 2, 3):
        below = shift(below, axis, 1)
        above = shift(above, axis, -1)
        pieces += [(below, -step, 0), (above, step, 0)]
    pieces += [(shift(below[:half], axis, 1), 4, 0), (shift(above[half:], axis, -1), 4, half)]
    return pieces


def spread(array, axis):
    size = lax.axis_size(axis)
    return exchange(jnp.broadcast_to(array[None], (size, *array.shape)), axis)


def rope_tables():
    half = HEAD // 2
    exponents = jnp.arange(half, dtype=jnp.float32) * (2.0 / HEAD)
    frequency = rope_base ** (-exponents)
    positions = jnp.arange(SEQ, dtype=jnp.int32).astype(jnp.float32)
    angles = positions[:, None] * frequency[None, :]
    cosine, sine = jnp.cos(angles), jnp.sin(angles)
    return (
        jnp.concatenate([cosine, cosine], axis=1),
        jnp.concatenate([-sine, sine], axis=1),
    )


def decoder(where, text, image, query_w, keyval_w, gain, cosine, sine):
    arrays, plan = [], []
    for pair, name in ((text, "t"), (image, "i")):
        for flip, a in enumerate(pair):
            plan += [(name, len(arrays), n, flip) for n in range(NY)]
            arrays.append(a)
    query_at = len(arrays)
    arrays.append(query_w)
    weights = []
    for a, parts in keyval_w:
        for dx, dz, row, rows, at in parts:
            weights.append((len(arrays), dx, dz, row, rows, at, 512, 256))
        arrays.append(a)
    count = len(arrays)
    n_act, n_w = len(plan), len(weights) + 1

    def kernel(where_ref, *refs):
        srcs = refs[:count]
        gain_ref, cos_ref, sin_ref = refs[count : count + 3]
        out_ref = refs[count + 3]
        a_ref, i_ref, b_ref, q_ref, act_sem, w_sem = refs[count + 4 :]
        x, z, y, c = where_ref[0], where_ref[1], where_ref[2], where_ref[3]
        start, n_rows = where_ref[4], where_ref[5]

        acts = []
        for k, (name, n, yy, flip) in enumerate(plan):
            side = yy if name == "i" else lax.rem(y + (0, 3, 1, 2)[yy], NY)
            t = side * NC + (c if flip == 0 else 1 - c)
            target = (a_ref if name == "t" else i_ref).at[t]
            acts.append(pltpu.make_async_copy(srcs[n].at[yy], target, act_sem.at[k]))
        for copy in acts:
            copy.start()
        loads = [
            pltpu.make_async_copy(srcs[query_at], b_ref.at[:, pl.ds(0, 512)], w_sem.at[len(weights)])
        ]
        for k, (n, dx, dz, row, rows, at, col, cols) in enumerate(weights):
            d = lax.rem(x + (dx + NX), NX) * NZ + lax.rem(z + (dz + NZ), NZ)
            first = pl.multiple_of(d * 256 + row, 64)
            loads.append(
                pltpu.make_async_copy(
                    srcs[n].at[pl.ds(at, rows), :],
                    b_ref.at[pl.ds(first, rows), pl.ds(col, cols)],
                    w_sem.at[k],
                )
            )
        for copy in loads:
            copy.start()
        for copy in acts:
            copy.wait()
        p_at = lax.broadcasted_iota(jnp.int32, (SEQ, SPAN), 0) - start
        j_at = lax.broadcasted_iota(jnp.int32, (SEQ, SPAN), 1)
        pick = jnp.where((p_at == j_at) & (j_at < n_rows), 1.0, 0.0).astype(jnp.bfloat16)
        rows_at = lax.broadcasted_iota(jnp.int32, (SEQ, 1), 0) - start
        is_image = (rows_at >= 0) & (rows_at < n_rows)

        def insert(t, total):
            placed = jnp.dot(pick, i_ref[t], preferred_element_type=jnp.float32)
            value = jnp.where(is_image, placed, a_ref[t].astype(jnp.float32))
            a_ref[t] = value.astype(jnp.bfloat16)
            return total + jnp.sum(value * value, axis=1, keepdims=True)

        total = lax.fori_loop(0, 8, insert, jnp.zeros((SEQ, 1), jnp.float32))
        scale = lax.rsqrt(total * (1.0 / WIDTH) + decoder_epsilon)

        def normalize(t, carry):
            a_ref[t] = (
                a_ref[t].astype(jnp.float32) * scale * gain_ref[pl.ds(t, 1), :]
            ).astype(jnp.bfloat16)
            return carry

        lax.fori_loop(0, 8, normalize, 0)
        for copy in loads:
            copy.wait()
        q_ref[...] = jnp.zeros(q_ref.shape, jnp.float32)

        def project(t, carry):
            q_ref[...] += jnp.dot(
                a_ref[t], b_ref[pl.ds(t * 1024, 1024), :], preferred_element_type=jnp.float32
            )
            return carry

        lax.fori_loop(0, 8, project, 0)
        cos, sin = cos_ref[...], sin_ref[...]

        def rotated(value):
            return (value * cos + pltpu.roll(value, 64, 1) * sin).astype(jnp.bfloat16)

        key = rotated(q_ref[:, 512:640])
        value = q_ref[:, 640:768].astype(jnp.bfloat16)
        causal = lax.broadcasted_iota(jnp.int32, (SEQ, SEQ), 0) >= lax.broadcasted_iota(
            jnp.int32, (SEQ, SEQ), 1
        )
        for h in range(4):
            query = rotated(q_ref[:, h * HEAD : (h + 1) * HEAD])
            scores = lax.dot_general(
                query, key, (((1,), (1,)), ((), ())), preferred_element_type=jnp.float32
            ) * (HEAD ** (-0.5))
            scores = jnp.where(causal, scores, -1e30)
            top = jnp.max(scores, axis=1, keepdims=True)
            e = jnp.exp(scores - top)
            w = (e / jnp.sum(e, axis=1, keepdims=True)).astype(jnp.bfloat16)
            out_ref[:, h * HEAD : (h + 1) * HEAD] = jnp.dot(
                w, value, preferred_element_type=jnp.float32
            ).astype(jnp.bfloat16)

    any_spec = pl.BlockSpec(memory_space=pl.ANY)
    vmem = pl.BlockSpec(memory_space=pltpu.VMEM)
    return pl.pallas_call(
        kernel,
        out_shape=jax.ShapeDtypeStruct((SEQ, 512), jnp.bfloat16),
        in_specs=[pl.BlockSpec(memory_space=pltpu.SMEM)] + [any_spec] * count + [vmem] * 3,
        out_specs=vmem,
        scratch_shapes=[
            pltpu.VMEM((8, SEQ, 1024), jnp.bfloat16),
            pltpu.VMEM((8, SPAN, 1024), jnp.bfloat16),
            pltpu.VMEM((WIDTH, 768), jnp.bfloat16),
            pltpu.VMEM((SEQ, 768), jnp.float32),
            pltpu.SemaphoreType.DMA((n_act,)),
            pltpu.SemaphoreType.DMA((n_w,)),
        ],
        compiler_params=pltpu.CompilerParams(vmem_limit_bytes=48 * 1024 * 1024),
        name="decoder",
    )(where, *arrays, gain, cosine, sine)


def vision(vis_rows, ln_gain, ln_bias, proj_weight, x, z, y, c):
    tokens = vis_rows.shape[0] * vis_rows.shape[1]
    own_w = jnp.swapaxes(proj_weight, 0, 1).reshape(200, 1024)
    below_w = shift(own_w, "x", 1)
    above_w = shift(own_w, "x", -1)
    far_w = shift(own_w, "x", 2)
    part = vis_rows.reshape(tokens, 2, 400).astype(jnp.float32)
    mean = jnp.mean(part, axis=(1, 2))
    dev = jnp.sum(jnp.square(part - mean[:, None, None]), axis=(1, 2))
    stats = jnp.stack([mean, dev])
    other = shift(stats, "c", 1)
    mean2 = (stats[0] + other[0]) * 0.5
    dev2 = stats[1] + other[1] + 400.0 * jnp.square(stats[0] - other[0])
    stats = jnp.stack([mean2, dev2])
    all_stats = jnp.stack([stats, shift(stats, "y", 1), shift(stats, "y", -1), shift(stats, "y", 2)])
    mean = jnp.mean(all_stats[:, 0], axis=0)
    variance = (
        jnp.sum(all_stats[:, 1], axis=0)
        + 1600.0 * jnp.sum(jnp.square(all_stats[:, 0] - mean[None]), axis=0)
    ) * (1.0 / 6400.0)
    t = y * NC + c
    gain = lax.dynamic_slice_in_dim(ln_gain, t * 400, 400, 1)
    bias = lax.dynamic_slice_in_dim(ln_bias, t * 400, 400, 1)
    normed = (
        (part - mean[:, None, None]) * lax.rsqrt(variance + vision_epsilon)[:, None, None] * gain
        + bias
    ).astype(jnp.bfloat16)
    blocks = jnp.moveaxis(normed.reshape(tokens, 2, 4, 100), 2, 0).reshape(4, tokens, 200)
    mask = (jnp.arange(2, dtype=jnp.int32) == c)[:, None, None, None, None]
    outgoing = jnp.where(mask, blocks[None, :, None], jnp.zeros((), jnp.bfloat16))
    outgoing = jnp.broadcast_to(outgoing, (2, 4, 2, tokens, 200)).reshape(16, tokens, 200)
    incoming = exchange(outgoing, ("z", "c")).reshape(8, 2, tokens, 200)
    mine = lax.dynamic_index_in_dim(incoming, z // 4, 1, keepdims=False).reshape(8 * tokens, 200)
    acts = spread(mine, "y")
    partial = None
    for dx, w in ((0, own_w), (-1, below_w), (1, above_w), (2, far_w)):
        a = lax.dynamic_index_in_dim(acts, lax.rem(x + dx + 4, 4), 0, keepdims=False)
        term = jnp.dot(a, w, preferred_element_type=jnp.float32)
        partial = term if partial is None else partial + term
    partial = partial.astype(jnp.bfloat16).reshape(8, tokens, 1024)
    parts = exchange(partial, "z")
    total = jnp.sum(parts.astype(jnp.float32), axis=0)
    return total.astype(jnp.bfloat16).reshape(8, 8, 1024)


def step(
    vis_rows, ln_gain, ln_bias, proj_weight, text_rows, attn_gain, w_query,
    key_value_weight, tile_counts, image_offsets,
):
    x, z = lax.axis_index("x"), lax.axis_index("z")
    y, c = lax.axis_index("y"), lax.axis_index("c")
    dp = x * NZ + z
    tile_ends = jnp.cumsum(tile_counts)
    tile_firsts = tile_ends - tile_counts
    sample_ids = jnp.arange(32, dtype=jnp.int32)
    tiles_here = jnp.arange(8, dtype=jnp.int32) * 32 + dp
    owners = jnp.sum((tile_ends[None, :] <= tiles_here[:, None]).astype(jnp.int32), axis=1)
    is_mine = sample_ids == dp
    my_first = jnp.sum(jnp.where(is_mine, tile_firsts, 0))
    my_count = jnp.sum(jnp.where(is_mine, tile_counts, 0))

    image = vision(vis_rows, ln_gain, ln_bias, proj_weight, x, z, y, c)

    pieces = ring4(text_rows[0], "y")
    own_text = jnp.concatenate([a for a, _, _ in pieces], axis=0).reshape(4, SEQ, 1024)
    text = (own_text, shift(own_text, "c", 1))

    query_w = lax.all_gather(w_query, ("x", "z"), axis=0, tiled=True)

    along_z = ring8(key_value_weight.reshape(256, 256), "z")
    stack = jnp.concatenate([a for a, _, _ in along_z], axis=0)
    offsets, at = [], 0
    for a, dz, row in along_z:
        offsets.append((dz, row, a.shape[0], at))
        at += a.shape[0]
    keyval_w = []
    for a, dx, first in ring4(stack, "x"):
        parts = [
            (dx, dz, row, rows, at - first)
            for dz, row, rows, at in offsets
            if first <= at and at + rows <= first + a.shape[0]
        ]
        keyval_w.append((a, parts))

    slots = jnp.zeros((32, 8, 1024), jnp.bfloat16)
    for r in range(8):
        slots = jnp.where((owners[r] == sample_ids)[:, None, None], image[r][None], slots)
    received = exchange(slots, ("x", "z"))
    sources = (my_first + jnp.arange(16, dtype=jnp.int32)) % 32
    mine = received[sources].reshape(SPAN, 1024)
    own_image = spread(mine, "y")
    image_all = (own_image, shift(own_image, "c", 1))

    where = jnp.stack([x, z, y, c, image_offsets[0], my_count * 8]).astype(jnp.int32)
    cosine, sine = rope_tables()
    out = decoder(
        where, text, image_all, query_w, keyval_w, attn_gain.reshape(8, 1024), cosine, sine
    )
    return out[None]


def solution(mesh):
    fine = Mesh(mesh.devices.reshape(NX, NZ, NY, NC), ("x", "z", "y", "c"))
    dp, tensor = ("x", "z"), ("y", "c")
    in_specs = (
        P(None, dp, None, tensor), P(), P(), P(dp, None, tensor), P(dp, None, tensor), P(),
        P(dp, tensor), P(dp, None, tensor), P(), P(dp),
    )
    return jax.shard_map(
        step, mesh=fine, in_specs=in_specs, out_specs=P(dp, None, tensor), check_vma=False
    )
```

```python
import jax
import jax.numpy as jnp
from jax import lax
from jax.experimental import pallas as pl
from jax.experimental.pallas import tpu as pltpu
from jax.sharding import Mesh, PartitionSpec as P


HEAD = 128
NX, NZ, NY, NC = 4, 8, 4, 2
SEQ = 384
SPAN = 128
WIDTH = 8192
COLS = 768
WIRE = COLS + 128
vision_epsilon = 1e-06
decoder_epsilon = 1e-05
rope_base = 500000.0


def shift(array, axis, by):
    size = lax.axis_size(axis)
    return lax.ppermute(array, axis, [(i, (i + by) % size) for i in range(size)])


def swap_xy(array):
    pairs = [(i * NY + j, j * NY + i) for i in range(NX) for j in range(NY)]
    return lax.ppermute(array, ("x", "y"), pairs)


def exchange(array, axis):
    return lax.all_to_all(array, axis, 0, 0, tiled=True)


def spread(array, axis):
    size = lax.axis_size(axis)
    return exchange(jnp.broadcast_to(array[None], (size, *array.shape)), axis)


def ring4(array, axis):
    half = array.shape[0] // 2
    below = shift(array, axis, 1)
    above = shift(array, axis, -1)
    far_low = shift(below[:half], axis, 1)
    far_high = shift(above[half:], axis, -1)
    return [(array, 0, 0), (below, -1, 0), (above, 1, 0), (far_low, 2, 0), (far_high, 2, half)]


def rope_tables():
    half = HEAD // 2
    exponents = jnp.arange(half, dtype=jnp.float32) * (2.0 / HEAD)
    frequency = rope_base ** (-exponents)
    positions = jnp.arange(SEQ, dtype=jnp.int32).astype(jnp.float32)
    angles = positions[:, None] * frequency[None, :]
    cosine, sine = jnp.cos(angles), jnp.sin(angles)
    return (
        jnp.concatenate([cosine, cosine], axis=1),
        jnp.concatenate([-sine, sine], axis=1),
    )


def project(where, pieces, weight, gain, rows, relative):
    arrays = [a for a, _ in pieces]
    plan = [(n, *part) for n, (_, parts) in enumerate(pieces) for part in parts]
    count = len(arrays)

    def kernel(where_ref, *refs):
        srcs, b_src, gain_ref, out_ref = refs[:count], refs[count], refs[count + 1], refs[count + 2]
        a_ref, b_ref, a_sem, b_sem = refs[count + 3 :]
        x, y, c = where_ref[0], where_ref[1], where_ref[2]
        loads = [pltpu.make_async_copy(b_src, b_ref, b_sem)]
        for k, (n, at, dy, sample, row, length, flip) in enumerate(plan):
            s = sample if dy is None else lax.rem(y + (dy + NY), NY)
            core = c if flip == 0 else 1 - c
            source = srcs[n] if at is None else srcs[n].at[at]
            target = a_ref.at[s, core, pl.ds(row, length), :]
            loads.append(pltpu.make_async_copy(source, target, a_sem.at[k]))
        for copy in loads:
            copy.start()
        for copy in loads:
            copy.wait()
        lane = lax.broadcasted_iota(jnp.int32, (rows, 128), 1)

        def one(s, carry):
            total = jnp.zeros((rows, 1), jnp.float32)
            acc = jnp.zeros((rows, COLS), jnp.float32)
            for core in range(NC):
                value = a_ref[s, core].astype(jnp.float32)
                total = total + jnp.sum(value * value, axis=1, keepdims=True)
                scaled = (value * gain_ref[core : core + 1, :]).astype(jnp.bfloat16)
                acc = acc + jnp.dot(
                    scaled, b_ref[core * 1024 : (core + 1) * 1024, :],
                    preferred_element_type=jnp.float32,
                )
            high = total.astype(jnp.bfloat16).astype(jnp.float32)
            low = total - high
            slot = lax.rem(s - x + NX, NX) if relative else s
            out_ref[slot, :, :COLS] = acc.astype(jnp.bfloat16)
            out_ref[slot, :, COLS:] = jnp.where(
                lane == 0, high, jnp.where(lane == 1, low, 0.0)
            ).astype(jnp.bfloat16)
            return carry

        lax.fori_loop(0, NX, one, 0)

    any_spec = pl.BlockSpec(memory_space=pl.ANY)
    vmem = pl.BlockSpec(memory_space=pltpu.VMEM)
    return pl.pallas_call(
        kernel,
        out_shape=jax.ShapeDtypeStruct((NX, rows, WIRE), jnp.bfloat16),
        in_specs=[pl.BlockSpec(memory_space=pltpu.SMEM)] + [any_spec] * (count + 1) + [vmem],
        out_specs=vmem,
        scratch_shapes=[
            pltpu.VMEM((NX, NC, rows, 1024), jnp.bfloat16),
            pltpu.VMEM((2048, COLS), jnp.bfloat16),
            pltpu.SemaphoreType.DMA((len(plan),)),
            pltpu.SemaphoreType.DMA,
        ],
        compiler_params=pltpu.CompilerParams(vmem_limit_bytes=40 * 1024 * 1024),
        cost_estimate=pl.CostEstimate(
            flops=2 * NX * rows * 2048 * COLS, bytes_accessed=10000000, transcendentals=0
        ),
    )(where, *arrays, weight, gain)


def attention(where, text_parts, image_parts, tables, image_tables):
    def kernel(where_ref, t0, t1, t2, t3, i_ref, cos_ref, sin_ref, icos_ref, isin_ref, out_ref):
        start, n_rows = where_ref[0], where_ref[1]

        def summed(parts):
            total = parts[0].astype(jnp.float32)
            for p in parts[1:]:
                total = total + p.astype(jnp.float32)
            squares = jnp.sum(total[:, COLS:], axis=1, keepdims=True)
            scale = lax.rsqrt(squares * (1.0 / WIDTH) + decoder_epsilon)
            return total[:, :COLS] * scale

        def heads(total, cos, sin):
            pieces = []
            for h in range(5):
                v = total[:, h * HEAD : (h + 1) * HEAD]
                pieces.append((v * cos + pltpu.roll(v, 64, 1) * sin).astype(jnp.bfloat16))
            pieces.append(total[:, 5 * HEAD :].astype(jnp.bfloat16))
            return pieces

        text = heads(summed([t0[...], t1[...], t2[...], t3[...]]), cos_ref[...], sin_ref[...])
        image = heads(summed([i_ref[n] for n in range(NX)]), icos_ref[...], isin_ref[...])
        p_at = lax.broadcasted_iota(jnp.int32, (SEQ, SPAN), 0) - start
        j_at = lax.broadcasted_iota(jnp.int32, (SEQ, SPAN), 1)
        pick = jnp.where((p_at == j_at) & (j_at < n_rows), 1.0, 0.0).astype(jnp.bfloat16)
        rows_at = lax.broadcasted_iota(jnp.int32, (SEQ, HEAD), 0) - start
        is_image = (rows_at >= 0) & (rows_at < n_rows)

        def merged(h):
            placed = jnp.dot(pick, image[h], preferred_element_type=jnp.float32)
            return jnp.where(is_image, placed, text[h].astype(jnp.float32)).astype(jnp.bfloat16)

        key, value = merged(4), merged(5)
        causal = lax.broadcasted_iota(jnp.int32, (SEQ, SEQ), 0) >= lax.broadcasted_iota(
            jnp.int32, (SEQ, SEQ), 1
        )
        for h in range(4):
            scores = lax.dot_general(
                merged(h), key, (((1,), (1,)), ((), ())), preferred_element_type=jnp.float32
            ) * (HEAD ** (-0.5))
            scores = jnp.where(causal, scores, -1e30)
            top = jnp.max(scores, axis=1, keepdims=True)
            e = jnp.exp(scores - top)
            w = (e / jnp.sum(e, axis=1, keepdims=True)).astype(jnp.bfloat16)
            out_ref[:, h * HEAD : (h + 1) * HEAD] = jnp.dot(
                w, value, preferred_element_type=jnp.float32
            ).astype(jnp.bfloat16)

    vmem = pl.BlockSpec(memory_space=pltpu.VMEM)
    return pl.pallas_call(
        kernel,
        out_shape=jax.ShapeDtypeStruct((SEQ, 512), jnp.bfloat16),
        in_specs=[pl.BlockSpec(memory_space=pltpu.SMEM)] + [vmem] * 9,
        out_specs=vmem,
        compiler_params=pltpu.CompilerParams(vmem_limit_bytes=40 * 1024 * 1024),
        name="attention",
    )(where, *text_parts, image_parts, *tables, *image_tables)


def vision(vis_rows, ln_gain, ln_bias, weight):
    tokens = vis_rows.shape[0] * vis_rows.shape[1]
    whole = spread(vis_rows.reshape(tokens, 2, 400), ("y", "c")).astype(jnp.float32)
    mean = jnp.mean(whole, axis=(0, 2, 3))[None, :, None, None]
    centered = whole - mean
    variance = jnp.mean(centered * centered, axis=(0, 2, 3))[None, :, None, None]
    gain = jnp.swapaxes(ln_gain.reshape(2, 8, 400), 0, 1)[:, None]
    bias = jnp.swapaxes(ln_bias.reshape(2, 8, 400), 0, 1)[:, None]
    normed = (centered * lax.rsqrt(variance + vision_epsilon) * gain + bias).astype(jnp.bfloat16)
    acts = exchange(normed.reshape(4, 2, tokens, 2, 400), "x")
    partial = jnp.einsum(
        "sctmf,cfmo->sto", acts, weight.reshape(2, 400, 2, 1024),
        preferred_element_type=jnp.float32,
    ).astype(jnp.bfloat16)
    parts = exchange(partial, "x")
    return jnp.sum(parts.astype(jnp.float32), axis=0).astype(jnp.bfloat16)


def step(
    vis_rows, ln_gain, ln_bias, proj_weight, text_rows, attn_gain, w_query,
    key_value_weight, tile_counts, image_offsets,
):
    x, z = lax.axis_index("x"), lax.axis_index("z")
    y, c = lax.axis_index("y"), lax.axis_index("c")
    tile_ends = jnp.cumsum(tile_counts)
    tile_firsts = tile_ends - tile_counts
    sample_ids = jnp.arange(32, dtype=jnp.int32)

    def entry(values, index):
        return jnp.sum(jnp.where(sample_ids == index, values, 0))

    proj_all = lax.all_gather(proj_weight, "z", axis=0, tiled=True)
    both = jnp.concatenate([w_query, key_value_weight.reshape(256, 256)], axis=1)
    both_all = lax.all_gather(both, "z", axis=0, tiled=True)

    image = vision(vis_rows, ln_gain, ln_bias, proj_all)

    turned = swap_xy(text_rows[0])
    own = ring4(turned, "y")
    text = []
    for a, dy, row in own:
        other = shift(a, "c", 1)
        text.append((a, [(None, dy, None, row, a.shape[0], 0)]))
        text.append((other, [(None, dy, None, row, a.shape[0], 1)]))

    image = swap_xy(image).reshape(8, 8, 1024)
    place = y * NZ + z
    tiles_here = jnp.arange(8, dtype=jnp.int32) * 32 + place
    owners = jnp.sum((tile_ends[None, :] <= tiles_here[:, None]).astype(jnp.int32), axis=1)
    slots = jnp.zeros((32, 8, 1024), jnp.bfloat16)
    for r in range(8):
        slots = jnp.where((owners[r] == sample_ids)[:, None, None], image[r][None], slots)
    received = exchange(slots, ("y", "z"))
    sources = (entry(tile_firsts, place) + jnp.arange(16, dtype=jnp.int32)) % 32
    mine = received[sources].reshape(SPAN, 1024)
    own_image = spread(mine, "y")
    other_image = shift(own_image, "c", 1)
    image_pieces = [
        (a, [(s, None, s, 0, SPAN, flip) for s in range(NX)])
        for flip, a in enumerate((own_image, other_image))
    ]

    gain = lax.dynamic_slice_in_dim(attn_gain, x * 2048, 2048).reshape(2, 1024)
    where = jnp.stack([x, y, c]).astype(jnp.int32)
    text_out = project(where, text, both_all, gain, SEQ, True)
    text_parts = [
        text_out[0],
        shift(text_out[1], "x", 1),
        shift(text_out[3], "x", -1),
        shift(text_out[2], "x", 2),
    ]
    image_out = project(where, image_pieces, both_all, gain, SPAN, False)
    image_parts = exchange(image_out, "x")

    tables = rope_tables()
    start = image_offsets[0]
    image_tables = [lax.dynamic_slice_in_dim(t, start, SPAN, 0) for t in tables]
    rows = entry(tile_counts, x * NZ + z) * 8
    out = attention(
        jnp.stack([start, rows]).astype(jnp.int32), text_parts, image_parts, tables, image_tables
    )
    return out[None]


def solution(mesh):
    fine = Mesh(mesh.devices.reshape(NX, NZ, NY, NC), ("x", "z", "y", "c"))
    dp, tensor = ("x", "z"), ("y", "c")
    in_specs = (
        P(None, dp, None, tensor), P(), P(), P(dp, None, tensor), P(dp, None, tensor), P(),
        P(dp, tensor), P(dp, None, tensor), P(), P(dp),
    )
    return jax.shard_map(
        step, mesh=fine, in_specs=in_specs, out_specs=P(dp, None, tensor), check_vma=False
    )
```

```python
import jax
import jax.numpy as jnp
from jax import lax
from jax.experimental import pallas as pl
from jax.experimental.pallas import tpu as pltpu
from jax.sharding import Mesh, PartitionSpec as P


HEAD = 128
NX, NZ, NY, NC = 4, 8, 4, 2
SEQ = 384
SPAN = 128
WIDTH = 8192
COLS = 768
WIRE = COLS + 128
vision_epsilon = 1e-06
decoder_epsilon = 1e-05
rope_base = 500000.0


def shift(array, axis, by):
    size = lax.axis_size(axis)
    return lax.ppermute(array, axis, [(i, (i + by) % size) for i in range(size)])


def swap_xy(array, flip=0):
    pairs = [(i * NY + j, j * NY + (i ^ flip)) for i in range(NX) for j in range(NY)]
    return lax.ppermute(array, ("x", "y"), pairs)


def exchange(array, axis):
    return lax.all_to_all(array, axis, 0, 0, tiled=True)


def spread(array, axis):
    size = lax.axis_size(axis)
    return exchange(jnp.broadcast_to(array[None], (size, *array.shape)), axis)


def ring4(array, axis):
    half = array.shape[0] // 2
    below = shift(array, axis, 1)
    above = shift(array, axis, -1)
    far_low = shift(below[:half], axis, 1)
    far_high = shift(above[half:], axis, -1)
    return [(array, 0, 0), (below, -1, 0), (above, 1, 0), (far_low, 2, 0), (far_high, 2, half)]


def rope_tables():
    half = HEAD // 2
    exponents = jnp.arange(half, dtype=jnp.float32) * (2.0 / HEAD)
    frequency = rope_base ** (-exponents)
    positions = jnp.arange(SEQ, dtype=jnp.int32).astype(jnp.float32)
    angles = positions[:, None] * frequency[None, :]
    cosine, sine = jnp.cos(angles), jnp.sin(angles)
    return (
        jnp.concatenate([cosine, cosine], axis=1),
        jnp.concatenate([-sine, sine], axis=1),
    )


def load_all(where_ref, plan, srcs, b_src, a_ref, b_ref, a_sem, b_sem):
    y, c = where_ref[1], where_ref[2]
    loads = [pltpu.make_async_copy(b_src, b_ref, b_sem)]
    for k, (n, at, dy, sample, row, length, flip) in enumerate(plan):
        s = sample if dy is None else lax.rem(y + (dy + NY), NY)
        core = c if flip == 0 else 1 - c
        source = srcs[n] if at is None else srcs[n].at[at]
        target = a_ref.at[s, core, pl.ds(row, length), :]
        loads.append(pltpu.make_async_copy(source, target, a_sem.at[k]))
    for copy in loads:
        copy.start()
    for copy in loads:
        copy.wait()


def project_text(where, pieces, weight):
    arrays = [a for a, _ in pieces]
    plan = [(n, *part) for n, (_, parts) in enumerate(pieces) for part in parts]
    count = len(arrays)
    half = SEQ // 2

    def kernel(where_ref, *refs):
        own_ref, up_ref, down_ref, a_ref, b_ref, a_sem, b_sem = refs[count + 1 :]
        load_all(where_ref, plan, refs[:count], refs[count], a_ref, b_ref, a_sem, b_sem)
        x = where_ref[0]
        for n in range(NX):
            s = lax.rem(x + n, NX)
            acc = jnp.dot(a_ref[s, 0], b_ref[:1024, :], preferred_element_type=jnp.float32)
            acc = acc + jnp.dot(a_ref[s, 1], b_ref[1024:, :], preferred_element_type=jnp.float32)
            acc = acc.astype(jnp.bfloat16)
            if n == 0:
                own_ref[...] = acc
            elif n == 1:
                up_ref[:SEQ, :] = acc
            elif n == 2:
                up_ref[SEQ:, :] = acc[:half]
                down_ref[:half, :] = acc[half:]
            else:
                down_ref[half:, :] = acc

    any_spec = pl.BlockSpec(memory_space=pl.ANY)
    vmem = pl.BlockSpec(memory_space=pltpu.VMEM)
    return pl.pallas_call(
        kernel,
        out_shape=[
            jax.ShapeDtypeStruct((n, COLS), jnp.bfloat16) for n in (SEQ, SEQ + half, SEQ + half)
        ],
        in_specs=[pl.BlockSpec(memory_space=pltpu.SMEM)] + [any_spec] * (count + 1),
        out_specs=[vmem] * 3,
        scratch_shapes=[
            pltpu.VMEM((NX, NC, SEQ, 1024), jnp.bfloat16),
            pltpu.VMEM((2048, COLS), jnp.bfloat16),
            pltpu.SemaphoreType.DMA((len(plan),)),
            pltpu.SemaphoreType.DMA,
        ],
        compiler_params=pltpu.CompilerParams(vmem_limit_bytes=40 * 1024 * 1024),
        name="project_text",
    )(where, *arrays, weight)


def project_image(where, pieces, weight, gain):
    arrays = [a for a, _ in pieces]
    plan = [(n, *part) for n, (_, parts) in enumerate(pieces) for part in parts]
    count = len(arrays)

    def kernel(where_ref, *refs):
        gain_ref, out_ref, a_ref, b_ref, a_sem, b_sem = refs[count + 1 :]
        load_all(where_ref, plan, refs[:count], refs[count], a_ref, b_ref, a_sem, b_sem)
        lane = lax.broadcasted_iota(jnp.int32, (SPAN, 128), 1)

        for s in range(NX):
            total = jnp.zeros((SPAN, 1), jnp.float32)
            acc = jnp.zeros((SPAN, COLS), jnp.float32)
            for core in range(NC):
                value = a_ref[s, core].astype(jnp.float32)
                total = total + jnp.sum(value * value, axis=1, keepdims=True)
                scaled = (value * gain_ref[core : core + 1, :]).astype(jnp.bfloat16)
                acc = acc + jnp.dot(
                    scaled, b_ref[core * 1024 : (core + 1) * 1024, :],
                    preferred_element_type=jnp.float32,
                )
            high = total.astype(jnp.bfloat16).astype(jnp.float32)
            low = total - high
            out_ref[s, :, :COLS] = acc.astype(jnp.bfloat16)
            out_ref[s, :, COLS:] = jnp.where(
                lane == 0, high, jnp.where(lane == 1, low, 0.0)
            ).astype(jnp.bfloat16)

    any_spec = pl.BlockSpec(memory_space=pl.ANY)
    vmem = pl.BlockSpec(memory_space=pltpu.VMEM)
    return pl.pallas_call(
        kernel,
        out_shape=jax.ShapeDtypeStruct((NX, SPAN, WIRE), jnp.bfloat16),
        in_specs=[pl.BlockSpec(memory_space=pltpu.SMEM)] + [any_spec] * (count + 1) + [vmem],
        out_specs=vmem,
        scratch_shapes=[
            pltpu.VMEM((NX, NC, SPAN, 1024), jnp.bfloat16),
            pltpu.VMEM((2048, COLS), jnp.bfloat16),
            pltpu.SemaphoreType.DMA((len(plan),)),
            pltpu.SemaphoreType.DMA,
        ],
        compiler_params=pltpu.CompilerParams(vmem_limit_bytes=40 * 1024 * 1024),
        name="project_image",
    )(where, *arrays, weight, gain)


def attention(where, text_parts, image_parts, tables, image_tables):
    half = SEQ // 2

    def kernel(
        where_ref, own, up, down, low, high, i_ref, cos_ref, sin_ref, icos_ref, isin_ref, out_ref
    ):
        start, n_rows = where_ref[0], where_ref[1]

        def wide(array):
            return array.astype(jnp.float32)

        text_sum = wide(own[...]) + wide(up[:SEQ]) + wide(down[half:])
        text_sum = jnp.concatenate(
            [text_sum[:half] + wide(low[...]), text_sum[half:] + wide(high[...])], axis=0
        )
        image_sum = wide(i_ref[0]) + wide(i_ref[1]) + wide(i_ref[2]) + wide(i_ref[3])
        squares = jnp.sum(image_sum[:, COLS:], axis=1, keepdims=True)
        image_sum = image_sum[:, :COLS] * lax.rsqrt(squares * (1.0 / WIDTH) + decoder_epsilon)

        def heads(total, cos, sin):
            pieces = []
            for h in range(5):
                v = total[:, h * HEAD : (h + 1) * HEAD]
                pieces.append((v * cos + pltpu.roll(v, 64, 1) * sin).astype(jnp.bfloat16))
            pieces.append(total[:, 5 * HEAD :].astype(jnp.bfloat16))
            return pieces

        text = heads(text_sum, cos_ref[...], sin_ref[...])
        image = heads(image_sum, icos_ref[...], isin_ref[...])
        p_at = lax.broadcasted_iota(jnp.int32, (SEQ, SPAN), 0) - start
        j_at = lax.broadcasted_iota(jnp.int32, (SEQ, SPAN), 1)
        pick = jnp.where((p_at == j_at) & (j_at < n_rows), 1.0, 0.0).astype(jnp.bfloat16)
        rows_at = lax.broadcasted_iota(jnp.int32, (SEQ, HEAD), 0) - start
        is_image = (rows_at >= 0) & (rows_at < n_rows)

        def merged(h):
            placed = jnp.dot(pick, image[h], preferred_element_type=jnp.float32)
            return jnp.where(is_image, placed, text[h].astype(jnp.float32)).astype(jnp.bfloat16)

        key, value = merged(4), merged(5)
        causal = lax.broadcasted_iota(jnp.int32, (SEQ, SEQ), 0) >= lax.broadcasted_iota(
            jnp.int32, (SEQ, SEQ), 1
        )
        for h in range(4):
            scores = lax.dot_general(
                merged(h), key, (((1,), (1,)), ((), ())), preferred_element_type=jnp.float32
            ) * (HEAD ** (-0.5))
            scores = jnp.where(causal, scores, -1e30)
            top = jnp.max(scores, axis=1, keepdims=True)
            e = jnp.exp(scores - top)
            w = (e / jnp.sum(e, axis=1, keepdims=True)).astype(jnp.bfloat16)
            out_ref[:, h * HEAD : (h + 1) * HEAD] = jnp.dot(
                w, value, preferred_element_type=jnp.float32
            ).astype(jnp.bfloat16)

    vmem = pl.BlockSpec(memory_space=pltpu.VMEM)
    return pl.pallas_call(
        kernel,
        out_shape=jax.ShapeDtypeStruct((SEQ, 512), jnp.bfloat16),
        in_specs=[pl.BlockSpec(memory_space=pltpu.SMEM)] + [vmem] * 10,
        out_specs=vmem,
        compiler_params=pltpu.CompilerParams(vmem_limit_bytes=40 * 1024 * 1024),
        name="attention",
    )(where, *text_parts, image_parts, *tables, *image_tables)


def vision(vis_rows, squares, ln_gain, ln_bias, weight):
    tokens = vis_rows.shape[0] * vis_rows.shape[1]
    parts, rest = [], squares
    for _ in range(3):
        parts.append(lax.reduce_precision(rest, 8, 7))
        rest = rest - parts[-1]
    rows = jnp.pad(jnp.stack(parts), ((0, 13), (0, 400 - SEQ))).astype(jnp.bfloat16)
    by_part = jnp.moveaxis(vis_rows, 2, 0).reshape(2 * tokens, 400)
    sent = jnp.concatenate([by_part, rows], axis=0)
    arrived = spread(sent, ("y", "c")).astype(jnp.float32)
    text_squares = jnp.sum(arrived[:, 2 * tokens : 2 * tokens + 3, :SEQ], axis=(0, 1))
    whole = arrived[:, : 2 * tokens].reshape(8, 2, tokens, 400)
    mean = jnp.mean(whole, axis=(0, 1, 3))[None, None, :, None]
    centered = whole - mean
    variance = jnp.mean(centered * centered, axis=(0, 1, 3))[None, None, :, None]
    gain = jnp.swapaxes(ln_gain.reshape(2, 8, 400), 0, 1)[:, :, None]
    bias = jnp.swapaxes(ln_bias.reshape(2, 8, 400), 0, 1)[:, :, None]
    normed = (centered * lax.rsqrt(variance + vision_epsilon) * gain + bias).astype(jnp.bfloat16)
    acts = exchange(normed.reshape(4, 2, 2, tokens, 400), "x")
    partial = jnp.einsum(
        "scmtf,cfmo->sto", acts, weight.reshape(2, 400, 2, 1024),
        preferred_element_type=jnp.float32,
    ).astype(jnp.bfloat16)
    total = None
    for k in range(NX):
        part = lax.dynamic_index_in_dim(partial, lax.axis_index("x") ^ k, 0, keepdims=False)
        part = swap_xy(part, k).astype(jnp.float32)
        total = part if total is None else total + part
    return total.astype(jnp.bfloat16), text_squares


def step(
    vis_rows, ln_gain, ln_bias, proj_weight, text_rows, attn_gain, w_query,
    key_value_weight, tile_counts, image_offsets,
):
    x, z = lax.axis_index("x"), lax.axis_index("z")
    y, c = lax.axis_index("y"), lax.axis_index("c")
    tile_ends = jnp.cumsum(tile_counts)
    tile_firsts = tile_ends - tile_counts
    sample_ids = jnp.arange(32, dtype=jnp.int32)

    def entry(values, index):
        return jnp.sum(jnp.where(sample_ids == index, values, 0))

    proj_all = lax.all_gather(proj_weight, "z", axis=0, tiled=True)
    both = jnp.concatenate([w_query, key_value_weight.reshape(256, 256)], axis=1)
    both_all = lax.all_gather(both, "z", axis=0, tiled=True)

    sequence = text_rows[0]
    wide = sequence.astype(jnp.float32)
    squares = jnp.sum(wide * wide, axis=1)
    image, squares = vision(vis_rows, squares, ln_gain, ln_bias, proj_all)
    scale = lax.rsqrt(squares * (1.0 / WIDTH) + decoder_epsilon)[:, None]
    own_gain = lax.dynamic_slice_in_dim(attn_gain, (y * NC + c) * 1024, 1024)
    normed = (wide * scale * own_gain[None]).astype(jnp.bfloat16)

    turned = swap_xy(normed)
    own = ring4(turned, "y")
    text = []
    for a, dy, row in own:
        other = shift(a, "c", 1)
        text.append((a, [(None, dy, None, row, a.shape[0], 0)]))
        text.append((other, [(None, dy, None, row, a.shape[0], 1)]))

    image = image.reshape(8, 8, 1024)
    place = y * NZ + z
    tiles_here = jnp.arange(8, dtype=jnp.int32) * 32 + place
    owners = jnp.sum((tile_ends[None, :] <= tiles_here[:, None]).astype(jnp.int32), axis=1)
    slots = jnp.zeros((32, 8, 1024), jnp.bfloat16)
    for r in range(8):
        slots = jnp.where((owners[r] == sample_ids)[:, None, None], image[r][None], slots)
    received = exchange(slots, ("y", "z"))
    sources = (entry(tile_firsts, place) + jnp.arange(16, dtype=jnp.int32)) % 32
    mine = received[sources].reshape(SPAN, 1024)
    own_image = spread(mine, "y")
    other_image = shift(own_image, "c", 1)
    image_pieces = [
        (a, [(s, None, s, 0, SPAN, flip) for s in range(NX)])
        for flip, a in enumerate((own_image, other_image))
    ]

    gain = lax.dynamic_slice_in_dim(attn_gain, x * 2048, 2048).reshape(2, 1024)
    where = jnp.stack([x, y, c]).astype(jnp.int32)
    own_sum, up, down = project_text(where, text, both_all)
    up = shift(up, "x", 1)
    down = shift(down, "x", -1)
    low = shift(up[SEQ:], "x", 1)
    high = shift(down[: SEQ // 2], "x", -1)
    text_parts = [own_sum, up, down, low, high]
    image_out = project_image(where, image_pieces, both_all, gain)
    image_parts = exchange(image_out, "x")

    tables = rope_tables()
    start = image_offsets[0]
    image_tables = [lax.dynamic_slice_in_dim(t, start, SPAN, 0) for t in tables]
    rows = entry(tile_counts, x * NZ + z) * 8
    out = attention(
        jnp.stack([start, rows]).astype(jnp.int32), text_parts, image_parts, tables, image_tables
    )
    return out[None]


def solution(mesh):
    fine = Mesh(mesh.devices.reshape(NX, NZ, NY, NC), ("x", "z", "y", "c"))
    dp, tensor = ("x", "z"), ("y", "c")
    in_specs = (
        P(None, dp, None, tensor), P(), P(), P(dp, None, tensor), P(dp, None, tensor), P(),
        P(dp, tensor), P(dp, None, tensor), P(), P(dp),
    )
    return jax.shard_map(
        step, mesh=fine, in_specs=in_specs, out_specs=P(dp, None, tensor), check_vma=False
    )
```

```python
import jax
import jax.numpy as jnp
from jax import lax
from jax.experimental import pallas as pl
from jax.experimental.pallas import tpu as pltpu
from jax.sharding import Mesh, PartitionSpec as P


HEAD = 128
NX, NZ, NY, NC = 4, 8, 4, 2
SEQ = 384
SPAN = 128
WIDTH = 8192
COLS = 768
WIRE = COLS + 128
vision_epsilon = 1e-06
decoder_epsilon = 1e-05
rope_base = 500000.0


def shift(array, axis, by):
    size = lax.axis_size(axis)
    return lax.ppermute(array, axis, [(i, (i + by) % size) for i in range(size)])


def swap_xy(array, flip=0):
    pairs = [(i * NY + j, (j ^ flip) * NY + i) for i in range(NX) for j in range(NY)]
    return lax.ppermute(array, ("x", "y"), pairs)


def flip_x(array, flip):
    return lax.ppermute(array, "x", [(i, i ^ flip) for i in range(NX)])


def exchange(array, axis):
    return lax.all_to_all(array, axis, 0, 0, tiled=True)


def spread(array, axis):
    size = lax.axis_size(axis)
    return exchange(jnp.broadcast_to(array[None], (size, *array.shape)), axis)


def ring4(array, axis):
    half = array.shape[0] // 2
    below = shift(array, axis, 1)
    above = shift(array, axis, -1)
    far_low = shift(below[:half], axis, 1)
    far_high = shift(above[half:], axis, -1)
    return [(array, 0, 0), (below, -1, 0), (above, 1, 0), (far_low, 2, 0), (far_high, 2, half)]


def rope_tables():
    half = HEAD // 2
    exponents = jnp.arange(half, dtype=jnp.float32) * (2.0 / HEAD)
    frequency = rope_base ** (-exponents)
    positions = jnp.arange(SEQ, dtype=jnp.int32).astype(jnp.float32)
    angles = positions[:, None] * frequency[None, :]
    cosine, sine = jnp.cos(angles), jnp.sin(angles)
    return (
        jnp.concatenate([cosine, cosine], axis=1),
        jnp.concatenate([-sine, sine], axis=1),
    )


def load_all(where_ref, plan, srcs, b_src, a_ref, b_ref, a_sem, b_sem):
    x, c = where_ref[0], where_ref[2]
    loads = [pltpu.make_async_copy(b_src, b_ref, b_sem)]
    for k, (n, at, dx, sample, row, length, flip) in enumerate(plan):
        s = sample if dx is None else lax.rem(x + (dx + NX), NX)
        core = c if flip == 0 else 1 - c
        source = srcs[n] if at is None else srcs[n].at[at]
        target = a_ref.at[s, core, pl.ds(row, length), :]
        loads.append(pltpu.make_async_copy(source, target, a_sem.at[k]))
    for copy in loads:
        copy.start()
    for copy in loads:
        copy.wait()


def project_text(where, pieces, weight, scale, gain):
    arrays = [a for a, _ in pieces]
    plan = [(n, *part) for n, (_, parts) in enumerate(pieces) for part in parts]
    count = len(arrays)

    def kernel(where_ref, *refs):
        scale_ref, gain_ref = refs[count + 1 : count + 3]
        outs = refs[count + 3 : count + 7]
        a_ref, b_ref, a_sem, b_sem = refs[count + 7 :]
        load_all(where_ref, plan, refs[:count], refs[count], a_ref, b_ref, a_sem, b_sem)
        y = where_ref[1]
        for n in range(NX):
            s = y ^ n
            acc = None
            for core in range(NC):
                normed = (
                    a_ref[s, core].astype(jnp.float32) * scale_ref[s] * gain_ref[core : core + 1, :]
                ).astype(jnp.bfloat16)
                term = jnp.dot(
                    normed, b_ref[core * 1024 : (core + 1) * 1024, :],
                    preferred_element_type=jnp.float32,
                )
                acc = term if acc is None else acc + term
            outs[n][...] = acc.astype(jnp.bfloat16)

    any_spec = pl.BlockSpec(memory_space=pl.ANY)
    vmem = pl.BlockSpec(memory_space=pltpu.VMEM)
    return pl.pallas_call(
        kernel,
        out_shape=[jax.ShapeDtypeStruct((SEQ, COLS), jnp.bfloat16)] * NX,
        in_specs=[pl.BlockSpec(memory_space=pltpu.SMEM)] + [any_spec] * (count + 1) + [vmem] * 2,
        out_specs=[vmem] * NX,
        scratch_shapes=[
            pltpu.VMEM((NX, NC, SEQ, 1024), jnp.bfloat16),
            pltpu.VMEM((2048, COLS), jnp.bfloat16),
            pltpu.SemaphoreType.DMA((len(plan),)),
            pltpu.SemaphoreType.DMA,
        ],
        compiler_params=pltpu.CompilerParams(vmem_limit_bytes=40 * 1024 * 1024),
        name="project_text",
    )(where, *arrays, weight, scale, gain)


def project_image(where, pieces, weight, gain):
    arrays = [a for a, _ in pieces]
    plan = [(n, *part) for n, (_, parts) in enumerate(pieces) for part in parts]
    count = len(arrays)

    def kernel(where_ref, *refs):
        gain_ref = refs[count + 1]
        outs = refs[count + 2 : count + 6]
        a_ref, b_ref, a_sem, b_sem = refs[count + 6 :]
        load_all(where_ref, plan, refs[:count], refs[count], a_ref, b_ref, a_sem, b_sem)
        y = where_ref[1]
        lane = lax.broadcasted_iota(jnp.int32, (SPAN, 128), 1)

        for n in range(NX):
            s = y ^ n
            total = jnp.zeros((SPAN, 1), jnp.float32)
            acc = jnp.zeros((SPAN, COLS), jnp.float32)
            for core in range(NC):
                value = a_ref[s, core].astype(jnp.float32)
                total = total + jnp.sum(value * value, axis=1, keepdims=True)
                scaled = (value * gain_ref[core : core + 1, :]).astype(jnp.bfloat16)
                acc = acc + jnp.dot(
                    scaled, b_ref[core * 1024 : (core + 1) * 1024, :],
                    preferred_element_type=jnp.float32,
                )
            high = total.astype(jnp.bfloat16).astype(jnp.float32)
            low = total - high
            outs[n][:, :COLS] = acc.astype(jnp.bfloat16)
            outs[n][:, COLS:] = jnp.where(
                lane == 0, high, jnp.where(lane == 1, low, 0.0)
            ).astype(jnp.bfloat16)

    any_spec = pl.BlockSpec(memory_space=pl.ANY)
    vmem = pl.BlockSpec(memory_space=pltpu.VMEM)
    return pl.pallas_call(
        kernel,
        out_shape=[jax.ShapeDtypeStruct((SPAN, WIRE), jnp.bfloat16)] * NX,
        in_specs=[pl.BlockSpec(memory_space=pltpu.SMEM)] + [any_spec] * (count + 1) + [vmem],
        out_specs=[vmem] * NX,
        scratch_shapes=[
            pltpu.VMEM((NX, NC, SPAN, 1024), jnp.bfloat16),
            pltpu.VMEM((2048, COLS), jnp.bfloat16),
            pltpu.SemaphoreType.DMA((len(plan),)),
            pltpu.SemaphoreType.DMA,
        ],
        compiler_params=pltpu.CompilerParams(vmem_limit_bytes=40 * 1024 * 1024),
        name="project_image",
    )(where, *arrays, weight, gain)


def attention(where, text_parts, image_parts, tables, image_tables):
    def kernel(where_ref, *refs):
        text_refs, image_refs = refs[:NX], refs[NX : 2 * NX]
        cos_ref, sin_ref, icos_ref, isin_ref, out_ref = refs[2 * NX :]
        start, n_rows = where_ref[0], where_ref[1]

        def summed(parts):
            total = parts[0][...].astype(jnp.float32)
            for p in parts[1:]:
                total = total + p[...].astype(jnp.float32)
            return total

        text_sum, image_sum = summed(text_refs), summed(image_refs)
        squares = jnp.sum(image_sum[:, COLS:], axis=1, keepdims=True)
        image_sum = image_sum[:, :COLS] * lax.rsqrt(squares * (1.0 / WIDTH) + decoder_epsilon)

        def heads(total, cos, sin):
            pieces = []
            for h in range(5):
                v = total[:, h * HEAD : (h + 1) * HEAD]
                pieces.append((v * cos + pltpu.roll(v, 64, 1) * sin).astype(jnp.bfloat16))
            pieces.append(total[:, 5 * HEAD :].astype(jnp.bfloat16))
            return pieces

        text = heads(text_sum, cos_ref[...], sin_ref[...])
        image = heads(image_sum, icos_ref[...], isin_ref[...])
        p_at = lax.broadcasted_iota(jnp.int32, (SEQ, SPAN), 0) - start
        j_at = lax.broadcasted_iota(jnp.int32, (SEQ, SPAN), 1)
        pick = jnp.where((p_at == j_at) & (j_at < n_rows), 1.0, 0.0).astype(jnp.bfloat16)
        rows_at = lax.broadcasted_iota(jnp.int32, (SEQ, HEAD), 0) - start
        is_image = (rows_at >= 0) & (rows_at < n_rows)

        def merged(h):
            placed = jnp.dot(pick, image[h], preferred_element_type=jnp.float32)
            return jnp.where(is_image, placed, text[h].astype(jnp.float32)).astype(jnp.bfloat16)

        key, value = merged(4), merged(5)
        causal = lax.broadcasted_iota(jnp.int32, (SEQ, SEQ), 0) >= lax.broadcasted_iota(
            jnp.int32, (SEQ, SEQ), 1
        )
        for h in range(4):
            scores = lax.dot_general(
                merged(h), key, (((1,), (1,)), ((), ())), preferred_element_type=jnp.float32
            ) * (HEAD ** (-0.5))
            scores = jnp.where(causal, scores, -1e30)
            top = jnp.max(scores, axis=1, keepdims=True)
            e = jnp.exp(scores - top)
            w = (e / jnp.sum(e, axis=1, keepdims=True)).astype(jnp.bfloat16)
            out_ref[:, h * HEAD : (h + 1) * HEAD] = jnp.dot(
                w, value, preferred_element_type=jnp.float32
            ).astype(jnp.bfloat16)

    vmem = pl.BlockSpec(memory_space=pltpu.VMEM)
    return pl.pallas_call(
        kernel,
        out_shape=jax.ShapeDtypeStruct((SEQ, 512), jnp.bfloat16),
        in_specs=[pl.BlockSpec(memory_space=pltpu.SMEM)] + [vmem] * (2 * NX + 4),
        out_specs=vmem,
        compiler_params=pltpu.CompilerParams(vmem_limit_bytes=40 * 1024 * 1024),
        name="attention",
    )(where, *text_parts, *image_parts, *tables, *image_tables)


def as_rows(values):
    parts, rest = [], values
    for _ in range(3):
        parts.append(lax.reduce_precision(rest, 8, 7))
        rest = rest - parts[-1]
    return jnp.pad(jnp.stack(parts), ((0, 13), (0, 400 - SEQ))).astype(jnp.bfloat16)


def vision(vis_rows, squares, ln_gain, ln_bias, weight):
    tokens = vis_rows.shape[0] * vis_rows.shape[1]
    rows = as_rows(squares)
    by_part = jnp.moveaxis(vis_rows, 2, 0).reshape(2 * tokens, 400)
    sent = jnp.concatenate([by_part, rows], axis=0)
    arrived = spread(sent, ("y", "c")).astype(jnp.float32)
    text_squares = jnp.sum(arrived[:, 2 * tokens : 2 * tokens + 3, :SEQ], axis=(0, 1))
    whole = arrived[:, : 2 * tokens].reshape(8, 2, tokens, 400)
    mean = jnp.mean(whole, axis=(0, 1, 3))[None, None, :, None]
    centered = whole - mean
    variance = jnp.mean(centered * centered, axis=(0, 1, 3))[None, None, :, None]
    gain = jnp.swapaxes(ln_gain.reshape(2, 8, 400), 0, 1)[:, :, None]
    bias = jnp.swapaxes(ln_bias.reshape(2, 8, 400), 0, 1)[:, :, None]
    normed = (centered * lax.rsqrt(variance + vision_epsilon) * gain + bias).astype(jnp.bfloat16)
    scale = lax.rsqrt(text_squares * (1.0 / WIDTH) + decoder_epsilon)
    rows = as_rows(scale)
    sent = jnp.concatenate(
        [normed.reshape(4, 4 * tokens, 400), jnp.broadcast_to(rows[None], (4, *rows.shape))], axis=1
    )
    acts = exchange(sent, "x")
    scales = jnp.sum(acts[:, 4 * tokens : 4 * tokens + 3, :SEQ].astype(jnp.float32), axis=1)
    acts = acts[:, : 4 * tokens].reshape(4, 2, 2, tokens, 400)
    partial = jnp.einsum(
        "scmtf,cfmo->sto", acts, weight.reshape(2, 400, 2, 1024),
        preferred_element_type=jnp.float32,
    ).astype(jnp.bfloat16)
    total = None
    for k in range(NX):
        part = lax.dynamic_index_in_dim(partial, lax.axis_index("x") ^ k, 0, keepdims=False)
        part = (part if k == 0 else flip_x(part, k)).astype(jnp.float32)
        total = part if total is None else total + part
    return total.astype(jnp.bfloat16), scales[:, :, None]


def step(
    vis_rows, ln_gain, ln_bias, proj_weight, text_rows, attn_gain, w_query,
    key_value_weight, tile_counts, image_offsets,
):
    x, z = lax.axis_index("x"), lax.axis_index("z")
    y, c = lax.axis_index("y"), lax.axis_index("c")
    tile_ends = jnp.cumsum(tile_counts)
    tile_firsts = tile_ends - tile_counts
    sample_ids = jnp.arange(32, dtype=jnp.int32)

    def entry(values, index):
        return jnp.sum(jnp.where(sample_ids == index, values, 0))

    proj_all = lax.all_gather(proj_weight, "z", axis=0, tiled=True)
    both = jnp.concatenate([w_query, key_value_weight.reshape(256, 256)], axis=1)
    both_all = lax.all_gather(swap_xy(both), "z", axis=0, tiled=True)

    sequence = text_rows[0]
    wide = sequence.astype(jnp.float32)
    squares = jnp.sum(wide * wide, axis=1)
    image, scales = vision(vis_rows, squares, ln_gain, ln_bias, proj_all)
    text = []
    for a, dx, row in ring4(sequence, "x"):
        other = shift(a, "c", 1)
        text.append((a, [(None, dx, None, row, a.shape[0], 0)]))
        text.append((other, [(None, dx, None, row, a.shape[0], 1)]))

    image = image.reshape(8, 8, 1024)
    place = x * NZ + z
    tiles_here = jnp.arange(8, dtype=jnp.int32) * 32 + place
    owners = jnp.sum((tile_ends[None, :] <= tiles_here[:, None]).astype(jnp.int32), axis=1)
    slots = jnp.zeros((32, 8, 1024), jnp.bfloat16)
    for r in range(8):
        slots = jnp.where((owners[r] == sample_ids)[:, None, None], image[r][None], slots)
    received = exchange(slots, ("x", "z"))
    sources = (entry(tile_firsts, place) + jnp.arange(16, dtype=jnp.int32)) % 32
    mine = received[sources].reshape(SPAN, 1024)
    own_image = spread(mine, "x")
    other_image = shift(own_image, "c", 1)
    image_pieces = [
        (a, [(s, None, s, 0, SPAN, flip) for s in range(NX)])
        for flip, a in enumerate((own_image, other_image))
    ]

    gain = lax.dynamic_slice_in_dim(attn_gain, y * 2048, 2048).reshape(2, 1024)
    where = jnp.stack([x, y, c]).astype(jnp.int32)
    text_parts = project_text(where, text, both_all, scales, gain)
    text_parts = [swap_xy(p, n) for n, p in enumerate(text_parts)]
    image_parts = project_image(where, image_pieces, both_all, gain)
    image_parts = [swap_xy(p, n) for n, p in enumerate(image_parts)]

    tables = rope_tables()
    start = image_offsets[0]
    image_tables = [lax.dynamic_slice_in_dim(t, start, SPAN, 0) for t in tables]
    rows = entry(tile_counts, place) * 8
    out = attention(
        jnp.stack([start, rows]).astype(jnp.int32), text_parts, image_parts, tables, image_tables
    )
    return out[None]


def solution(mesh):
    fine = Mesh(mesh.devices.reshape(NX, NZ, NY, NC), ("x", "z", "y", "c"))
    dp, tensor = ("x", "z"), ("y", "c")
    in_specs = (
        P(None, dp, None, tensor), P(), P(), P(dp, None, tensor), P(dp, None, tensor), P(),
        P(dp, tensor), P(dp, None, tensor), P(), P(dp),
    )
    return jax.shard_map(
        step, mesh=fine, in_specs=in_specs, out_specs=P(dp, None, tensor), check_vma=False
    )
```

```python
import jax
import jax.numpy as jnp
from jax import lax
from jax.experimental import pallas as pl
from jax.experimental.pallas import tpu as pltpu
from jax.sharding import Mesh, PartitionSpec as P


HEAD = 128
NX, NZ, NY, NC = 4, 8, 4, 2
SEQ = 384
SPAN = 128
WIDTH = 8192
COLS = 768
WIRE = COLS + 128
vision_epsilon = 1e-06
decoder_epsilon = 1e-05
rope_base = 500000.0


def shift(array, axis, by):
    size = lax.axis_size(axis)
    return lax.ppermute(array, axis, [(i, (i + by) % size) for i in range(size)])


def swap_xy(array, flip=0):
    pairs = [(i * NY + j, (j ^ flip) * NY + i) for i in range(NX) for j in range(NY)]
    return lax.ppermute(array, ("x", "y"), pairs)


def flip_x(array, flip):
    return lax.ppermute(array, "x", [(i, i ^ flip) for i in range(NX)])


def exchange(array, axis):
    return lax.all_to_all(array, axis, 0, 0, tiled=True)


def spread(array, axis):
    size = lax.axis_size(axis)
    return exchange(jnp.broadcast_to(array[None], (size, *array.shape)), axis)


def ring4(array, axis):
    half = array.shape[0] // 2
    below = shift(array, axis, 1)
    above = shift(array, axis, -1)
    far_low = shift(below[:half], axis, 1)
    far_high = shift(above[half:], axis, -1)
    return [(array, 0, 0), (below, -1, 0), (above, 1, 0), (far_low, 2, 0), (far_high, 2, half)]


def rope_tables():
    half = HEAD // 2
    exponents = jnp.arange(half, dtype=jnp.float32) * (2.0 / HEAD)
    frequency = rope_base ** (-exponents)
    positions = jnp.arange(SEQ, dtype=jnp.int32).astype(jnp.float32)
    angles = positions[:, None] * frequency[None, :]
    cosine, sine = jnp.cos(angles), jnp.sin(angles)
    return (
        jnp.concatenate([cosine, cosine], axis=1),
        jnp.concatenate([-sine, sine], axis=1),
    )


def load_all(where_ref, plan, srcs, b_src, a_ref, b_ref, a_sem, b_sem):
    x, c = where_ref[0], where_ref[2]
    loads = [pltpu.make_async_copy(b_src, b_ref, b_sem)]
    for k, (n, at, dx, sample, row, length, flip) in enumerate(plan):
        s = sample if dx is None else lax.rem(x + (dx + NX), NX)
        core = c if flip == 0 else 1 - c
        source = srcs[n] if at is None else srcs[n].at[at]
        target = a_ref.at[s, core, pl.ds(row, length), :]
        loads.append(pltpu.make_async_copy(source, target, a_sem.at[k]))
    for copy in loads:
        copy.start()
    for copy in loads:
        copy.wait()


def project_text(where, pieces, weight):
    arrays = [a for a, _ in pieces]
    plan = [(n, *part) for n, (_, parts) in enumerate(pieces) for part in parts]
    count = len(arrays)

    def kernel(where_ref, *refs):
        outs = refs[count + 1 : count + 5]
        a_ref, b_ref, a_sem, b_sem = refs[count + 5 :]
        load_all(where_ref, plan, refs[:count], refs[count], a_ref, b_ref, a_sem, b_sem)
        y = where_ref[1]
        for n in range(NX):
            s = y ^ n
            acc = jnp.dot(a_ref[s, 0], b_ref[:1024, :], preferred_element_type=jnp.float32)
            acc = acc + jnp.dot(a_ref[s, 1], b_ref[1024:, :], preferred_element_type=jnp.float32)
            outs[n][...] = acc.astype(jnp.bfloat16)

    any_spec = pl.BlockSpec(memory_space=pltpu.HBM)
    vmem = pl.BlockSpec(memory_space=pltpu.VMEM)
    return pl.pallas_call(
        kernel,
        out_shape=[jax.ShapeDtypeStruct((SEQ, COLS), jnp.bfloat16)] * NX,
        in_specs=[pl.BlockSpec(memory_space=pltpu.SMEM)] + [any_spec] * (count + 1),
        out_specs=[vmem] * NX,
        scratch_shapes=[
            pltpu.VMEM((NX, NC, SEQ, 1024), jnp.bfloat16),
            pltpu.VMEM((2048, COLS), jnp.bfloat16),
            pltpu.SemaphoreType.DMA((len(plan),)),
            pltpu.SemaphoreType.DMA,
        ],
        compiler_params=pltpu.CompilerParams(vmem_limit_bytes=40 * 1024 * 1024),
        name="project_text",
    )(where, *arrays, weight)


def project_image(where, pieces, weight, gain):
    arrays = [a for a, _ in pieces]
    plan = [(n, *part) for n, (_, parts) in enumerate(pieces) for part in parts]
    count = len(arrays)

    def kernel(where_ref, *refs):
        gain_ref = refs[count + 1]
        outs = refs[count + 2 : count + 6]
        a_ref, b_ref, a_sem, b_sem = refs[count + 6 :]
        load_all(where_ref, plan, refs[:count], refs[count], a_ref, b_ref, a_sem, b_sem)
        y = where_ref[1]
        lane = lax.broadcasted_iota(jnp.int32, (SPAN, 128), 1)

        for n in range(NX):
            s = y ^ n
            total = jnp.zeros((SPAN, 1), jnp.float32)
            acc = jnp.zeros((SPAN, COLS), jnp.float32)
            for core in range(NC):
                value = a_ref[s, core].astype(jnp.float32)
                total = total + jnp.sum(value * value, axis=1, keepdims=True)
                scaled = (value * gain_ref[core : core + 1, :]).astype(jnp.bfloat16)
                acc = acc + jnp.dot(
                    scaled, b_ref[core * 1024 : (core + 1) * 1024, :],
                    preferred_element_type=jnp.float32,
                )
            high = total.astype(jnp.bfloat16).astype(jnp.float32)
            low = total - high
            outs[n][:, :COLS] = acc.astype(jnp.bfloat16)
            outs[n][:, COLS:] = jnp.where(
                lane == 0, high, jnp.where(lane == 1, low, 0.0)
            ).astype(jnp.bfloat16)

    any_spec = pl.BlockSpec(memory_space=pltpu.HBM)
    vmem = pl.BlockSpec(memory_space=pltpu.VMEM)
    return pl.pallas_call(
        kernel,
        out_shape=[jax.ShapeDtypeStruct((SPAN, WIRE), jnp.bfloat16)] * NX,
        in_specs=[pl.BlockSpec(memory_space=pltpu.SMEM)] + [any_spec] * (count + 1) + [vmem],
        out_specs=[vmem] * NX,
        scratch_shapes=[
            pltpu.VMEM((NX, NC, SPAN, 1024), jnp.bfloat16),
            pltpu.VMEM((2048, COLS), jnp.bfloat16),
            pltpu.SemaphoreType.DMA((len(plan),)),
            pltpu.SemaphoreType.DMA,
        ],
        compiler_params=pltpu.CompilerParams(vmem_limit_bytes=40 * 1024 * 1024),
        name="project_image",
    )(where, *arrays, weight, gain)


def attention(where, text_parts, image_parts, tables, image_tables):
    def kernel(where_ref, *refs):
        text_refs, image_refs = refs[:NX], refs[NX : 2 * NX]
        cos_ref, sin_ref, icos_ref, isin_ref, out_ref = refs[2 * NX :]
        start, n_rows = where_ref[0], where_ref[1]

        def summed(parts):
            total = parts[0][...].astype(jnp.float32)
            for p in parts[1:]:
                total = total + p[...].astype(jnp.float32)
            return total

        text_sum, image_sum = summed(text_refs), summed(image_refs)
        squares = jnp.sum(image_sum[:, COLS:], axis=1, keepdims=True)
        image_sum = image_sum[:, :COLS] * lax.rsqrt(squares * (1.0 / WIDTH) + decoder_epsilon)

        def heads(total, cos, sin):
            pieces = []
            for h in range(5):
                v = total[:, h * HEAD : (h + 1) * HEAD]
                pieces.append((v * cos + pltpu.roll(v, 64, 1) * sin).astype(jnp.bfloat16))
            pieces.append(total[:, 5 * HEAD :].astype(jnp.bfloat16))
            return pieces

        text = heads(text_sum, cos_ref[...], sin_ref[...])
        image = heads(image_sum, icos_ref[...], isin_ref[...])
        p_at = lax.broadcasted_iota(jnp.int32, (SEQ, SPAN), 0) - start
        j_at = lax.broadcasted_iota(jnp.int32, (SEQ, SPAN), 1)
        pick = jnp.where((p_at == j_at) & (j_at < n_rows), 1.0, 0.0).astype(jnp.bfloat16)
        rows_at = lax.broadcasted_iota(jnp.int32, (SEQ, HEAD), 0) - start
        is_image = (rows_at >= 0) & (rows_at < n_rows)

        def merged(h):
            placed = jnp.dot(pick, image[h], preferred_element_type=jnp.float32)
            return jnp.where(is_image, placed, text[h].astype(jnp.float32)).astype(jnp.bfloat16)

        key, value = merged(4), merged(5)
        causal = lax.broadcasted_iota(jnp.int32, (SEQ, SEQ), 0) >= lax.broadcasted_iota(
            jnp.int32, (SEQ, SEQ), 1
        )
        for h in range(4):
            scores = lax.dot_general(
                merged(h), key, (((1,), (1,)), ((), ())), preferred_element_type=jnp.float32
            ) * (HEAD ** (-0.5))
            scores = jnp.where(causal, scores, -1e30)
            top = jnp.max(scores, axis=1, keepdims=True)
            e = jnp.exp(scores - top)
            w = (e / jnp.sum(e, axis=1, keepdims=True)).astype(jnp.bfloat16)
            out_ref[:, h * HEAD : (h + 1) * HEAD] = jnp.dot(
                w, value, preferred_element_type=jnp.float32
            ).astype(jnp.bfloat16)

    vmem = pl.BlockSpec(memory_space=pltpu.VMEM)
    return pl.pallas_call(
        kernel,
        out_shape=jax.ShapeDtypeStruct((SEQ, 512), jnp.bfloat16),
        in_specs=[pl.BlockSpec(memory_space=pltpu.SMEM)] + [vmem] * (2 * NX + 4),
        out_specs=vmem,
        compiler_params=pltpu.CompilerParams(vmem_limit_bytes=40 * 1024 * 1024),
        name="attention",
    )(where, *text_parts, *image_parts, *tables, *image_tables)


def as_rows(values):
    parts, rest = [], values
    for _ in range(3):
        parts.append(lax.reduce_precision(rest, 8, 7))
        rest = rest - parts[-1]
    return jnp.pad(jnp.stack(parts), ((0, 13), (0, 400 - SEQ))).astype(jnp.bfloat16)


def layer_norm(arrived, gain, bias):
    tokens = 64

    def kernel(in_ref, gain_ref, bias_ref, out_ref):
        def read(t, m):
            return in_ref[t, m * tokens : (m + 1) * tokens, :].astype(jnp.float32)

        parts = [(t, m) for t in range(8) for m in range(2)]
        total = jnp.zeros((tokens, 1), jnp.float32)
        for t, m in parts:
            total = total + jnp.sum(read(t, m), axis=1, keepdims=True)
        mean = total * (1.0 / 6400)
        total = jnp.zeros((tokens, 1), jnp.float32)
        for t, m in parts:
            centered = read(t, m) - mean
            total = total + jnp.sum(centered * centered, axis=1, keepdims=True)
        scale = lax.rsqrt(total * (1.0 / 6400) + vision_epsilon)
        for t, m in parts:
            value = (read(t, m) - mean) * scale * gain_ref[t, m : m + 1, :]
            out_ref[t, m * tokens : (m + 1) * tokens, :] = (
                value + bias_ref[t, m : m + 1, :]
            ).astype(jnp.bfloat16)

    vmem = pl.BlockSpec(memory_space=pltpu.VMEM)
    return pl.pallas_call(
        kernel,
        out_shape=jax.ShapeDtypeStruct((8, 2 * tokens, 400), jnp.bfloat16),
        in_specs=[vmem] * 3,
        out_specs=vmem,
        name="layer_norm",
    )(arrived, gain, bias)


def vision(vis_rows, squares, ln_gain, ln_bias, weight):
    tokens = vis_rows.shape[0] * vis_rows.shape[1]
    by_part = jnp.moveaxis(vis_rows, 2, 0).reshape(2 * tokens, 400)
    sent = jnp.concatenate([by_part, as_rows(squares)], axis=0)
    arrived = spread(sent, ("y", "c"))
    squares = jnp.sum(
        arrived[:, 2 * tokens : 2 * tokens + 3, :SEQ].astype(jnp.float32), axis=(0, 1)
    )
    gain = jnp.swapaxes(ln_gain.reshape(2, 8, 400), 0, 1)
    bias = jnp.swapaxes(ln_bias.reshape(2, 8, 400), 0, 1)
    normed = layer_norm(arrived, gain, bias)
    acts = exchange(normed.reshape(4, 2, 2, tokens, 400), "x")
    partial = jnp.einsum(
        "scmtf,cfmo->sto", acts, weight.reshape(2, 400, 2, 1024),
        preferred_element_type=jnp.float32,
    ).astype(jnp.bfloat16)
    total = None
    for k in range(NX):
        part = lax.dynamic_index_in_dim(partial, lax.axis_index("x") ^ k, 0, keepdims=False)
        part = (part if k == 0 else flip_x(part, k)).astype(jnp.float32)
        total = part if total is None else total + part
    return total.astype(jnp.bfloat16), squares


def step(
    vis_rows, ln_gain, ln_bias, proj_weight, text_rows, attn_gain, w_query,
    key_value_weight, tile_counts, image_offsets,
):
    x, z = lax.axis_index("x"), lax.axis_index("z")
    y, c = lax.axis_index("y"), lax.axis_index("c")
    tile_ends = jnp.cumsum(tile_counts)
    tile_firsts = tile_ends - tile_counts
    sample_ids = jnp.arange(32, dtype=jnp.int32)

    def entry(values, index):
        return jnp.sum(jnp.where(sample_ids == index, values, 0))

    proj_all = lax.all_gather(proj_weight, "z", axis=0, tiled=True)
    both = jnp.concatenate([w_query, key_value_weight.reshape(256, 256)], axis=1)
    both_all = lax.all_gather(swap_xy(both), "z", axis=0, tiled=True)

    sequence = text_rows[0]
    wide = sequence.astype(jnp.float32)
    squares = jnp.sum(wide * wide, axis=1)
    image, squares = vision(vis_rows, squares, ln_gain, ln_bias, proj_all)
    scale = lax.rsqrt(squares * (1.0 / WIDTH) + decoder_epsilon)[:, None]
    own_gain = lax.dynamic_slice_in_dim(attn_gain, (y * NC + c) * 1024, 1024)
    normed = (wide * scale * own_gain[None]).astype(jnp.bfloat16)
    text = []
    for a, dx, row in ring4(normed, "x"):
        other = shift(a, "c", 1)
        text.append((a, [(None, dx, None, row, a.shape[0], 0)]))
        text.append((other, [(None, dx, None, row, a.shape[0], 1)]))

    image = image.reshape(8, 8, 1024)
    place = x * NZ + z
    tiles_here = jnp.arange(8, dtype=jnp.int32) * 32 + place
    owners = jnp.sum((tile_ends[None, :] <= tiles_here[:, None]).astype(jnp.int32), axis=1)
    slots = jnp.zeros((32, 8, 1024), jnp.bfloat16)
    for r in range(8):
        slots = jnp.where((owners[r] == sample_ids)[:, None, None], image[r][None], slots)
    received = exchange(slots, ("x", "z"))
    sources = (entry(tile_firsts, place) + jnp.arange(16, dtype=jnp.int32)) % 32
    mine = received[sources].reshape(SPAN, 1024)
    own_image = spread(mine, "x")
    other_image = shift(own_image, "c", 1)
    image_pieces = [
        (a, [(s, None, s, 0, SPAN, flip) for s in range(NX)])
        for flip, a in enumerate((own_image, other_image))
    ]

    gain = lax.dynamic_slice_in_dim(attn_gain, y * 2048, 2048).reshape(2, 1024)
    where = jnp.stack([x, y, c]).astype(jnp.int32)
    text_parts = project_text(where, text, both_all)
    text_parts = [swap_xy(p, n) for n, p in enumerate(text_parts)]
    image_parts = project_image(where, image_pieces, both_all, gain)
    image_parts = [swap_xy(p, n) for n, p in enumerate(image_parts)]

    tables = rope_tables()
    start = image_offsets[0]
    image_tables = [lax.dynamic_slice_in_dim(t, start, SPAN, 0) for t in tables]
    rows = entry(tile_counts, place) * 8
    out = attention(
        jnp.stack([start, rows]).astype(jnp.int32), text_parts, image_parts, tables, image_tables
    )
    return out[None]


def solution(mesh):
    fine = Mesh(mesh.devices.reshape(NX, NZ, NY, NC), ("x", "z", "y", "c"))
    dp, tensor = ("x", "z"), ("y", "c")
    in_specs = (
        P(None, dp, None, tensor), P(), P(), P(dp, None, tensor), P(dp, None, tensor), P(),
        P(dp, tensor), P(dp, None, tensor), P(), P(dp),
    )
    return jax.shard_map(
        step, mesh=fine, in_specs=in_specs, out_specs=P(dp, None, tensor), check_vma=False
    )
```

```python
import jax
import jax.numpy as jnp
from jax import lax
from jax.experimental import pallas as pl
from jax.experimental.pallas import tpu as pltpu
from jax.sharding import Mesh, PartitionSpec as P


HEAD = 128
NX, NZ, NY, NC = 4, 8, 4, 2
SEQ = 384
SPAN = 128
WIDTH = 8192
vision_epsilon = 1e-06
decoder_epsilon = 1e-05
rope_base = 500000.0


def shift(array, axis, by):
    size = lax.axis_size(axis)
    return lax.ppermute(array, axis, [(i, (i + by) % size) for i in range(size)])


def flip_x(array, flip):
    return lax.ppermute(array, "x", [(i, i ^ flip) for i in range(NX)])


def exchange(array, axis):
    return lax.all_to_all(array, axis, 0, 0, tiled=True)


def spread(array, axis):
    size = lax.axis_size(axis)
    return exchange(jnp.broadcast_to(array[None], (size, *array.shape)), axis)


def ring4(array, axis):
    half = array.shape[0] // 2
    below = shift(array, axis, 1)
    above = shift(array, axis, -1)
    far_low = shift(below[:half], axis, 1)
    far_high = shift(above[half:], axis, -1)
    return [(array, 0, 0), (below, -1, 0), (above, 1, 0), (far_low, 2, 0), (far_high, 2, half)]


def ring8(array, axis):
    half = array.shape[0] // 2
    pieces = [(array, 0, 0)]
    below = above = array
    for step in (1, 2, 3):
        below = shift(below, axis, 1)
        above = shift(above, axis, -1)
        pieces += [(below, -step, 0), (above, step, 0)]
    pieces += [(shift(below[:half], axis, 1), 4, 0), (shift(above[half:], axis, -1), 4, half)]
    return pieces


def rope_tables():
    half = HEAD // 2
    exponents = jnp.arange(half, dtype=jnp.float32) * (2.0 / HEAD)
    frequency = rope_base ** (-exponents)
    positions = jnp.arange(SEQ, dtype=jnp.int32).astype(jnp.float32)
    angles = positions[:, None] * frequency[None, :]
    cosine, sine = jnp.cos(angles), jnp.sin(angles)
    return (
        jnp.concatenate([cosine, cosine], axis=1),
        jnp.concatenate([-sine, sine], axis=1),
    )


VMEM = pl.BlockSpec(memory_space=pltpu.VMEM)
SMEM = pl.BlockSpec(memory_space=pltpu.SMEM)
HBM = pl.BlockSpec(memory_space=pltpu.HBM)


def pack(pieces):
    rows = sum(a.shape[0] for a in pieces)

    def kernel(*refs):
        at = 0
        for ref in refs[:-1]:
            refs[-1][at : at + ref.shape[0], :] = ref[...]
            at += ref.shape[0]

    return pl.pallas_call(
        kernel,
        out_shape=jax.ShapeDtypeStruct((rows, pieces[0].shape[1]), pieces[0].dtype),
        in_specs=[VMEM] * len(pieces),
        out_specs=VMEM,
        name="pack",
    )(*pieces)


def rotated(value, cos, sin):
    return (value * cos + pltpu.roll(value, 64, 1) * sin).astype(jnp.bfloat16)


def prepare(where, text, image, keyval, gain, cosine, sine):
    arrays = [a for a, _, _, _ in text] + list(image) + [a for a, _ in keyval]
    n_text, count = len(text), len(arrays)
    plan = [
        (n_text + 2 + n, *part) for n, (_, parts) in enumerate(keyval) for part in parts
    ]

    def kernel(where_ref, *refs):
        gain_ref, cos_ref, sin_ref = refs[count : count + 3]
        a_ref, key_ref, value_ref = refs[count + 3 : count + 6]
        b_ref, sem = refs[count + 6 :]
        x, z, y, c = where_ref[0], where_ref[1], where_ref[2], where_ref[3]
        start, n_rows = where_ref[4], where_ref[5]
        loads = []
        for k, (n, dx, dz, row, rows, at) in enumerate(plan):
            d = lax.rem(x + (dx + NX), NX) * NZ + lax.rem(z + (dz + NZ), NZ)
            first = pl.multiple_of(d * 256 + row, 128)
            loads.append(
                pltpu.make_async_copy(
                    refs[n].at[pl.ds(at, rows), :], b_ref.at[pl.ds(first, rows), :], sem.at[k]
                )
            )
        for copy in loads:
            copy.start()

        total = {}
        for n, (_, dy, first, flip) in enumerate(text):
            rows = refs[n].shape[0]
            side = lax.rem(y + (dy + NY), NY)
            t = side * NC + (c if flip == 0 else 1 - c)
            p_at = lax.broadcasted_iota(jnp.int32, (rows, SPAN), 0) + first - start
            j_at = lax.broadcasted_iota(jnp.int32, (rows, SPAN), 1)
            pick = jnp.where((p_at == j_at) & (j_at < n_rows), 1.0, 0.0).astype(jnp.bfloat16)
            rows_at = lax.broadcasted_iota(jnp.int32, (rows, 1), 0) + first - start
            is_image = (rows_at >= 0) & (rows_at < n_rows)
            placed = jnp.dot(
                pick, refs[n_text + flip][side], preferred_element_type=jnp.float32
            )
            value = jnp.where(is_image, placed, refs[n][...].astype(jnp.float32))
            a_ref[t, first : first + rows, :] = value.astype(jnp.bfloat16)
            squares = jnp.sum(value * value, axis=1, keepdims=True)
            if rows < SEQ:
                zero = jnp.zeros((SEQ - rows, 1), jnp.float32)
                squares = jnp.concatenate([squares, zero] if first == 0 else [zero, squares], axis=0)
            total = squares if n == 0 else total + squares
        scale = lax.rsqrt(total * (1.0 / WIDTH) + decoder_epsilon)
        for copy in loads:
            copy.wait()
        acc = jnp.zeros((SEQ, 256), jnp.float32)
        for t in range(8):
            normed = (
                a_ref[t].astype(jnp.float32) * scale * gain_ref[t : t + 1, :]
            ).astype(jnp.bfloat16)
            a_ref[t] = normed
            acc = acc + jnp.dot(
                normed, b_ref[t * 1024 : (t + 1) * 1024, :], preferred_element_type=jnp.float32
            )
        key_ref[...] = rotated(acc[:, :HEAD], cos_ref[...], sin_ref[...])
        value_ref[...] = acc[:, HEAD:].astype(jnp.bfloat16)

    return pl.pallas_call(
        kernel,
        out_shape=[
            jax.ShapeDtypeStruct((8, SEQ, 1024), jnp.bfloat16),
            jax.ShapeDtypeStruct((SEQ, HEAD), jnp.bfloat16),
            jax.ShapeDtypeStruct((SEQ, HEAD), jnp.bfloat16),
        ],
        in_specs=[SMEM] + [VMEM] * (n_text + 2) + [HBM] * len(keyval) + [VMEM] * 3,
        out_specs=[VMEM] * 3,
        scratch_shapes=[
            pltpu.VMEM((WIDTH, 256), jnp.bfloat16),
            pltpu.SemaphoreType.DMA((len(plan),)),
        ],
        compiler_params=pltpu.CompilerParams(vmem_limit_bytes=48 * 1024 * 1024),
        name="prepare",
    )(where, *arrays, gain, cosine, sine)


def attention(sequence, query_w, key, value, cosine, sine):
    def kernel(a_ref, w_hbm, key_ref, value_ref, cos_ref, sin_ref, out_ref, w_ref, sem):
        loads = [
            pltpu.make_async_copy(
                w_hbm.at[pl.ds(t * 1024, 1024), :], w_ref.at[pl.ds(t * 1024, 1024), :], sem.at[t]
            )
            for t in range(8)
        ]
        for copy in loads:
            copy.start()
        acc = jnp.zeros((SEQ, 512), jnp.float32)
        for t in range(8):
            loads[t].wait()
            acc = acc + jnp.dot(
                a_ref[t], w_ref[t * 1024 : (t + 1) * 1024, :], preferred_element_type=jnp.float32
            )
        cos, sin = cos_ref[...], sin_ref[...]
        causal = lax.broadcasted_iota(jnp.int32, (SEQ, SEQ), 0) >= lax.broadcasted_iota(
            jnp.int32, (SEQ, SEQ), 1
        )
        for h in range(4):
            query = rotated(acc[:, h * HEAD : (h + 1) * HEAD], cos, sin)
            scores = lax.dot_general(
                query, key_ref[...], (((1,), (1,)), ((), ())), preferred_element_type=jnp.float32
            ) * (HEAD ** (-0.5))
            scores = jnp.where(causal, scores, -1e30)
            top = jnp.max(scores, axis=1, keepdims=True)
            e = jnp.exp(scores - top)
            w = (e / jnp.sum(e, axis=1, keepdims=True)).astype(jnp.bfloat16)
            out_ref[:, h * HEAD : (h + 1) * HEAD] = jnp.dot(
                w, value_ref[...], preferred_element_type=jnp.float32
            ).astype(jnp.bfloat16)

    return pl.pallas_call(
        kernel,
        out_shape=jax.ShapeDtypeStruct((SEQ, 512), jnp.bfloat16),
        in_specs=[VMEM, HBM] + [VMEM] * 4,
        out_specs=VMEM,
        scratch_shapes=[
            pltpu.VMEM((WIDTH, 512), jnp.bfloat16),
            pltpu.SemaphoreType.DMA((8,)),
        ],
        compiler_params=pltpu.CompilerParams(vmem_limit_bytes=48 * 1024 * 1024),
        name="attention",
    )(sequence, query_w, key, value, cosine, sine)


def vision(vis_rows, ln_gain, ln_bias, weight):
    tokens = vis_rows.shape[0] * vis_rows.shape[1]
    whole = spread(vis_rows.reshape(tokens, 2, 400), ("y", "c")).astype(jnp.float32)
    mean = jnp.mean(whole, axis=(0, 2, 3))[None, :, None, None]
    centered = whole - mean
    variance = jnp.mean(centered * centered, axis=(0, 2, 3))[None, :, None, None]
    gain = jnp.swapaxes(ln_gain.reshape(2, 8, 400), 0, 1)[:, None]
    bias = jnp.swapaxes(ln_bias.reshape(2, 8, 400), 0, 1)[:, None]
    normed = (centered * lax.rsqrt(variance + vision_epsilon) * gain + bias).astype(jnp.bfloat16)
    acts = exchange(normed.reshape(4, 2, tokens, 2, 400), "x")
    partial = jnp.einsum(
        "sctmf,cfmo->sto", acts, weight.reshape(2, 400, 2, 1024),
        preferred_element_type=jnp.float32,
    ).astype(jnp.bfloat16)
    total = None
    for k in range(NX):
        part = lax.dynamic_index_in_dim(partial, lax.axis_index("x") ^ k, 0, keepdims=False)
        part = (part if k == 0 else flip_x(part, k)).astype(jnp.float32)
        total = part if total is None else total + part
    return total.astype(jnp.bfloat16)


def step(
    vis_rows, ln_gain, ln_bias, proj_weight, text_rows, attn_gain, w_query,
    key_value_weight, tile_counts, image_offsets,
):
    x, z = lax.axis_index("x"), lax.axis_index("z")
    y, c = lax.axis_index("y"), lax.axis_index("c")
    tile_ends = jnp.cumsum(tile_counts)
    tile_firsts = tile_ends - tile_counts
    sample_ids = jnp.arange(32, dtype=jnp.int32)

    def entry(values, index):
        return jnp.sum(jnp.where(sample_ids == index, values, 0))

    proj_all = lax.all_gather(proj_weight, "z", axis=0, tiled=True)
    query_w = lax.all_gather(w_query, ("x", "z"), axis=0, tiled=True)

    image = vision(vis_rows, ln_gain, ln_bias, proj_all).reshape(8, 8, 1024)

    along_z = ring8(key_value_weight.reshape(256, 256), "z")
    offsets, at = [], 0
    for a, dz, row in along_z:
        offsets.append((dz, row, a.shape[0], at))
        at += a.shape[0]
    keyval = []
    for a, dx, first in ring4(pack([a for a, _, _ in along_z]), "x"):
        parts = [
            (dx, dz, row, rows, at - first)
            for dz, row, rows, at in offsets
            if first <= at and at + rows <= first + a.shape[0]
        ]
        keyval.append((a, parts))

    text = []
    for a, dy, row in ring4(text_rows[0], "y"):
        text.append((a, dy, row, 0))
        text.append((shift(a, "c", 1), dy, row, 1))

    place = x * NZ + z
    tiles_here = jnp.arange(8, dtype=jnp.int32) * 32 + place
    owners = jnp.sum((tile_ends[None, :] <= tiles_here[:, None]).astype(jnp.int32), axis=1)
    slots = jnp.zeros((32, 8, 1024), jnp.bfloat16)
    for r in range(8):
        slots = jnp.where((owners[r] == sample_ids)[:, None, None], image[r][None], slots)
    received = exchange(slots, ("x", "z"))
    sources = (entry(tile_firsts, place) + jnp.arange(16, dtype=jnp.int32)) % 32
    mine = received[sources].reshape(SPAN, 1024)
    own_image = spread(mine, "y")
    other_image = shift(own_image, "c", 1)

    rows = entry(tile_counts, place) * 8
    where = jnp.stack([x, z, y, c, image_offsets[0], rows]).astype(jnp.int32)
    cosine, sine = rope_tables()
    sequence, key, value = prepare(
        where, text, (own_image, other_image), keyval, attn_gain.reshape(8, 1024), cosine, sine
    )
    return attention(sequence, query_w, key, value, cosine, sine)[None]


def solution(mesh):
    fine = Mesh(mesh.devices.reshape(NX, NZ, NY, NC), ("x", "z", "y", "c"))
    dp, tensor = ("x", "z"), ("y", "c")
    in_specs = (
        P(None, dp, None, tensor), P(), P(), P(dp, None, tensor), P(dp, None, tensor), P(),
        P(dp, tensor), P(dp, None, tensor), P(), P(dp),
    )
    return jax.shard_map(
        step, mesh=fine, in_specs=in_specs, out_specs=P(dp, None, tensor), check_vma=False
    )
```

```python
import jax
import jax.numpy as jnp
from jax import lax
from jax.experimental import pallas as pl
from jax.experimental.pallas import tpu as pltpu
from jax.sharding import Mesh, PartitionSpec as P


HEAD = 128
NX, NZ, NY, NC = 4, 8, 4, 2
SEQ = 384
SPAN = 128
WIDTH = 8192
vision_epsilon = 1e-06
decoder_epsilon = 1e-05
rope_base = 500000.0


def shift(array, axis, by):
    size = lax.axis_size(axis)
    return lax.ppermute(array, axis, [(i, (i + by) % size) for i in range(size)])


def flip_x(array, flip):
    return lax.ppermute(array, "x", [(i, i ^ flip) for i in range(NX)])


def exchange(array, axis):
    return lax.all_to_all(array, axis, 0, 0, tiled=True)


def spread(array, axis):
    size = lax.axis_size(axis)
    return exchange(jnp.broadcast_to(array[None], (size, *array.shape)), axis)


def ring4(array, axis):
    half = array.shape[0] // 2
    below = shift(array, axis, 1)
    above = shift(array, axis, -1)
    far_low = shift(below[:half], axis, 1)
    far_high = shift(above[half:], axis, -1)
    return [(array, 0, 0), (below, -1, 0), (above, 1, 0), (far_low, 2, 0), (far_high, 2, half)]


def ring8(array, axis):
    half = array.shape[0] // 2
    pieces = [(array, 0, 0)]
    below = above = array
    for step in (1, 2, 3):
        below = shift(below, axis, 1)
        above = shift(above, axis, -1)
        pieces += [(below, -step, 0), (above, step, 0)]
    pieces += [(shift(below[:half], axis, 1), 4, 0), (shift(above[half:], axis, -1), 4, half)]
    return pieces


def rope_tables():
    half = HEAD // 2
    exponents = jnp.arange(half, dtype=jnp.float32) * (2.0 / HEAD)
    frequency = rope_base ** (-exponents)
    positions = jnp.arange(SEQ, dtype=jnp.int32).astype(jnp.float32)
    angles = positions[:, None] * frequency[None, :]
    cosine, sine = jnp.cos(angles), jnp.sin(angles)
    return (
        jnp.concatenate([cosine, cosine], axis=1),
        jnp.concatenate([-sine, sine], axis=1),
    )


VMEM = pl.BlockSpec(memory_space=pltpu.VMEM)
SMEM = pl.BlockSpec(memory_space=pltpu.SMEM)
HBM = pl.BlockSpec(memory_space=pltpu.HBM)


def pack(pieces):
    rows = sum(a.shape[0] for a in pieces)

    def kernel(*refs):
        at = 0
        for ref in refs[:-1]:
            refs[-1][at : at + ref.shape[0], :] = ref[...]
            at += ref.shape[0]

    return pl.pallas_call(
        kernel,
        out_shape=jax.ShapeDtypeStruct((rows, pieces[0].shape[1]), pieces[0].dtype),
        in_specs=[VMEM] * len(pieces),
        out_specs=VMEM,
        name="pack",
    )(*pieces)


def rotated(value, cos, sin):
    return (value * cos + pltpu.roll(value, 64, 1) * sin).astype(jnp.bfloat16)


def one_head(query, key, value):
    at = lax.broadcasted_iota(jnp.int32, (SEQ, SEQ), 0)
    causal = at >= lax.broadcasted_iota(jnp.int32, (SEQ, SEQ), 1)
    scores = lax.dot_general(
        query, key, (((1,), (1,)), ((), ())), preferred_element_type=jnp.float32
    ) * (HEAD ** (-0.5))
    scores = jnp.where(causal, scores, -1e30)
    top = jnp.max(scores, axis=1, keepdims=True)
    e = jnp.exp(scores - top)
    w = (e / jnp.sum(e, axis=1, keepdims=True)).astype(jnp.bfloat16)
    return jnp.dot(w, value, preferred_element_type=jnp.float32).astype(jnp.bfloat16)


def prepare(where, text, image, keyval, gain, cosine, sine):
    arrays = [a for a, _, _, _ in text] + list(image) + [a for a, _ in keyval]
    n_text, count = len(text), len(arrays)
    plan = [
        (n_text + 2 + n, *part) for n, (_, parts) in enumerate(keyval) for part in parts
    ]

    def kernel(where_ref, *refs):
        gain_ref, cos_ref, sin_ref = refs[count : count + 3]
        a_ref, key_ref, value_ref, last_ref = refs[count + 3 : count + 7]
        b_ref, sem = refs[count + 7 :]
        x, z, y, c = where_ref[0], where_ref[1], where_ref[2], where_ref[3]
        start, n_rows = where_ref[4], where_ref[5]
        loads = []
        for k, (n, dx, dz, row, rows, at) in enumerate(plan):
            d = lax.rem(x + (dx + NX), NX) * NZ + lax.rem(z + (dz + NZ), NZ)
            first = pl.multiple_of(d * 256 + row, 128)
            loads.append(
                pltpu.make_async_copy(
                    refs[n].at[pl.ds(at, rows), :], b_ref.at[pl.ds(first, rows), :], sem.at[k]
                )
            )
        for copy in loads:
            copy.start()

        total = {}
        for n, (_, dy, first, flip) in enumerate(text):
            rows = refs[n].shape[0]
            side = lax.rem(y + (dy + NY), NY)
            t = side * NC + (c if flip == 0 else 1 - c)
            p_at = lax.broadcasted_iota(jnp.int32, (rows, SPAN), 0) + first - start
            j_at = lax.broadcasted_iota(jnp.int32, (rows, SPAN), 1)
            pick = jnp.where((p_at == j_at) & (j_at < n_rows), 1.0, 0.0).astype(jnp.bfloat16)
            rows_at = lax.broadcasted_iota(jnp.int32, (rows, 1), 0) + first - start
            is_image = (rows_at >= 0) & (rows_at < n_rows)
            placed = jnp.dot(
                pick, refs[n_text + flip][side], preferred_element_type=jnp.float32
            )
            value = jnp.where(is_image, placed, refs[n][...].astype(jnp.float32))
            a_ref[t, first : first + rows, :] = value.astype(jnp.bfloat16)
            squares = jnp.sum(value * value, axis=1, keepdims=True)
            if rows < SEQ:
                zero = jnp.zeros((SEQ - rows, 1), jnp.float32)
                squares = jnp.concatenate([squares, zero] if first == 0 else [zero, squares], axis=0)
            total = squares if n == 0 else total + squares
        scale = lax.rsqrt(total * (1.0 / WIDTH) + decoder_epsilon)
        for copy in loads:
            copy.wait()
        acc = jnp.zeros((SEQ, 384), jnp.float32)
        for t in range(8):
            normed = (
                a_ref[t].astype(jnp.float32) * scale * gain_ref[t : t + 1, :]
            ).astype(jnp.bfloat16)
            a_ref[t] = normed
            acc = acc + jnp.dot(
                normed, b_ref[t * 1024 : (t + 1) * 1024, :], preferred_element_type=jnp.float32
            )
        cos, sin = cos_ref[...], sin_ref[...]
        key = rotated(acc[:, :HEAD], cos, sin)
        value = acc[:, HEAD : 2 * HEAD].astype(jnp.bfloat16)
        key_ref[...] = key
        value_ref[...] = value
        last_ref[...] = one_head(rotated(acc[:, 2 * HEAD :], cos, sin), key, value)

    return pl.pallas_call(
        kernel,
        out_shape=[
            jax.ShapeDtypeStruct((8, SEQ, 1024), jnp.bfloat16),
        ]
        + [jax.ShapeDtypeStruct((SEQ, HEAD), jnp.bfloat16)] * 3,
        in_specs=[SMEM] + [VMEM] * (n_text + 2) + [HBM] * len(keyval) + [VMEM] * 3,
        out_specs=[VMEM] * 4,
        scratch_shapes=[
            pltpu.VMEM((WIDTH, 384), jnp.bfloat16),
            pltpu.SemaphoreType.DMA((len(plan),)),
        ],
        compiler_params=pltpu.CompilerParams(vmem_limit_bytes=48 * 1024 * 1024),
        name="prepare",
    )(where, *arrays, gain, cosine, sine)


def attention(sequence, query_w, key, value, last, cosine, sine):
    def kernel(a_ref, w_hbm, key_ref, value_ref, last_ref, cos_ref, sin_ref, out_ref, w_ref, sem):
        loads = [
            pltpu.make_async_copy(
                w_hbm.at[pl.ds(t * 1024, 1024), :], w_ref.at[pl.ds(t * 1024, 1024), :], sem.at[t]
            )
            for t in range(8)
        ]
        for copy in loads:
            copy.start()
        acc = jnp.zeros((SEQ, 384), jnp.float32)
        for t in range(8):
            loads[t].wait()
            acc = acc + jnp.dot(
                a_ref[t], w_ref[t * 1024 : (t + 1) * 1024, :], preferred_element_type=jnp.float32
            )
        cos, sin = cos_ref[...], sin_ref[...]
        for h in range(3):
            query = rotated(acc[:, h * HEAD : (h + 1) * HEAD], cos, sin)
            out_ref[:, h * HEAD : (h + 1) * HEAD] = one_head(query, key_ref[...], value_ref[...])
        out_ref[:, 3 * HEAD :] = last_ref[...]

    return pl.pallas_call(
        kernel,
        out_shape=jax.ShapeDtypeStruct((SEQ, 512), jnp.bfloat16),
        in_specs=[VMEM, HBM] + [VMEM] * 5,
        out_specs=VMEM,
        scratch_shapes=[
            pltpu.VMEM((WIDTH, 384), jnp.bfloat16),
            pltpu.SemaphoreType.DMA((8,)),
        ],
        compiler_params=pltpu.CompilerParams(vmem_limit_bytes=48 * 1024 * 1024),
        name="attention",
    )(sequence, query_w, key, value, last, cosine, sine)


def vision(vis_rows, ln_gain, ln_bias, weight):
    tokens = vis_rows.shape[0] * vis_rows.shape[1]
    whole = spread(vis_rows.reshape(tokens, 2, 400), ("y", "c")).astype(jnp.float32)
    mean = jnp.mean(whole, axis=(0, 2, 3))[None, :, None, None]
    centered = whole - mean
    variance = jnp.mean(centered * centered, axis=(0, 2, 3))[None, :, None, None]
    gain = jnp.swapaxes(ln_gain.reshape(2, 8, 400), 0, 1)[:, None]
    bias = jnp.swapaxes(ln_bias.reshape(2, 8, 400), 0, 1)[:, None]
    normed = (centered * lax.rsqrt(variance + vision_epsilon) * gain + bias).astype(jnp.bfloat16)
    acts = exchange(normed.reshape(4, 2, tokens, 2, 400), "x")
    partial = jnp.einsum(
        "sctmf,cfmo->sto", acts, weight.reshape(2, 400, 2, 1024),
        preferred_element_type=jnp.float32,
    ).astype(jnp.bfloat16)
    total = None
    for k in range(NX):
        part = lax.dynamic_index_in_dim(partial, lax.axis_index("x") ^ k, 0, keepdims=False)
        part = (part if k == 0 else flip_x(part, k)).astype(jnp.float32)
        total = part if total is None else total + part
    return total.astype(jnp.bfloat16)


def step(
    vis_rows, ln_gain, ln_bias, proj_weight, text_rows, attn_gain, w_query,
    key_value_weight, tile_counts, image_offsets,
):
    x, z = lax.axis_index("x"), lax.axis_index("z")
    y, c = lax.axis_index("y"), lax.axis_index("c")
    tile_ends = jnp.cumsum(tile_counts)
    tile_firsts = tile_ends - tile_counts
    sample_ids = jnp.arange(32, dtype=jnp.int32)

    def entry(values, index):
        return jnp.sum(jnp.where(sample_ids == index, values, 0))

    proj_all = lax.all_gather(proj_weight, "z", axis=0, tiled=True)
    query_w = lax.all_gather(w_query[:, : 3 * HEAD], ("x", "z"), axis=0, tiled=True)

    image = vision(vis_rows, ln_gain, ln_bias, proj_all).reshape(8, 8, 1024)

    mixed = jnp.concatenate(
        [key_value_weight.reshape(256, 256), w_query[:, 3 * HEAD :]], axis=1
    )
    along_z = ring8(mixed, "z")
    offsets, at = [], 0
    for a, dz, row in along_z:
        offsets.append((dz, row, a.shape[0], at))
        at += a.shape[0]
    keyval = []
    for a, dx, first in ring4(pack([a for a, _, _ in along_z]), "x"):
        parts = [
            (dx, dz, row, rows, at - first)
            for dz, row, rows, at in offsets
            if first <= at and at + rows <= first + a.shape[0]
        ]
        keyval.append((a, parts))

    text = []
    for a, dy, row in ring4(text_rows[0], "y"):
        text.append((a, dy, row, 0))
        text.append((shift(a, "c", 1), dy, row, 1))

    place = x * NZ + z
    tiles_here = jnp.arange(8, dtype=jnp.int32) * 32 + place
    owners = jnp.sum((tile_ends[None, :] <= tiles_here[:, None]).astype(jnp.int32), axis=1)
    slots = jnp.zeros((32, 8, 1024), jnp.bfloat16)
    for r in range(8):
        slots = jnp.where((owners[r] == sample_ids)[:, None, None], image[r][None], slots)
    received = exchange(slots, ("x", "z"))
    sources = (entry(tile_firsts, place) + jnp.arange(16, dtype=jnp.int32)) % 32
    mine = received[sources].reshape(SPAN, 1024)
    own_image = spread(mine, "y")
    other_image = shift(own_image, "c", 1)

    rows = entry(tile_counts, place) * 8
    where = jnp.stack([x, z, y, c, image_offsets[0], rows]).astype(jnp.int32)
    cosine, sine = rope_tables()
    sequence, key, value, last = prepare(
        where, text, (own_image, other_image), keyval, attn_gain.reshape(8, 1024), cosine, sine
    )
    return attention(sequence, query_w, key, value, last, cosine, sine)[None]


def solution(mesh):
    fine = Mesh(mesh.devices.reshape(NX, NZ, NY, NC), ("x", "z", "y", "c"))
    dp, tensor = ("x", "z"), ("y", "c")
    in_specs = (
        P(None, dp, None, tensor), P(), P(), P(dp, None, tensor), P(dp, None, tensor), P(),
        P(dp, tensor), P(dp, None, tensor), P(), P(dp),
    )
    return jax.shard_map(
        step, mesh=fine, in_specs=in_specs, out_specs=P(dp, None, tensor), check_vma=False
    )
```

```python
import jax
import jax.numpy as jnp
from jax import lax
from jax.experimental import pallas as pl
from jax.experimental.pallas import tpu as pltpu
from jax.sharding import Mesh, PartitionSpec as P


HEAD = 128
NX, NZ, NY, NC = 4, 8, 4, 2
SEQ = 384
SPAN = 128
WIDTH = 8192
vision_epsilon = 1e-06
decoder_epsilon = 1e-05
rope_base = 500000.0


def shift(array, axis, by):
    size = lax.axis_size(axis)
    return lax.ppermute(array, axis, [(i, (i + by) % size) for i in range(size)])


def flip_x(array, flip):
    return lax.ppermute(array, "x", [(i, i ^ flip) for i in range(NX)])


def exchange(array, axis):
    return lax.all_to_all(array, axis, 0, 0, tiled=True)


def spread(array, axis):
    size = lax.axis_size(axis)
    return exchange(jnp.broadcast_to(array[None], (size, *array.shape)), axis)


def ring4(array, axis):
    half = array.shape[0] // 2
    below = shift(array, axis, 1)
    above = shift(array, axis, -1)
    far_low = shift(below[:half], axis, 1)
    far_high = shift(above[half:], axis, -1)
    return [(array, 0, 0), (below, -1, 0), (above, 1, 0), (far_low, 2, 0), (far_high, 2, half)]


def ring8(array, axis):
    half = array.shape[0] // 2
    pieces = [(array, 0, 0)]
    below = above = array
    for step in (1, 2, 3):
        below = shift(below, axis, 1)
        above = shift(above, axis, -1)
        pieces += [(below, -step, 0), (above, step, 0)]
    pieces += [(shift(below[:half], axis, 1), 4, 0), (shift(above[half:], axis, -1), 4, half)]
    return pieces


def rope_tables():
    half = HEAD // 2
    exponents = jnp.arange(half, dtype=jnp.float32) * (2.0 / HEAD)
    frequency = rope_base ** (-exponents)
    positions = jnp.arange(SEQ, dtype=jnp.int32).astype(jnp.float32)
    angles = positions[:, None] * frequency[None, :]
    cosine, sine = jnp.cos(angles), jnp.sin(angles)
    return (
        jnp.concatenate([cosine, cosine], axis=1),
        jnp.concatenate([-sine, sine], axis=1),
    )


VMEM = pl.BlockSpec(memory_space=pltpu.VMEM)
SMEM = pl.BlockSpec(memory_space=pltpu.SMEM)
HBM = pl.BlockSpec(memory_space=pltpu.HBM)


def pack(pieces):
    rows = sum(a.shape[0] for a in pieces)

    def kernel(*refs):
        at = 0
        for ref in refs[:-1]:
            refs[-1][at : at + ref.shape[0], :] = ref[...]
            at += ref.shape[0]

    return pl.pallas_call(
        kernel,
        out_shape=jax.ShapeDtypeStruct((rows, pieces[0].shape[1]), pieces[0].dtype),
        in_specs=[VMEM] * len(pieces),
        out_specs=VMEM,
        name="pack",
    )(*pieces)


def rotated(value, cos, sin):
    return (value * cos + pltpu.roll(value, 64, 1) * sin).astype(jnp.bfloat16)


def prepare(where, text, image, keyval, gain, cosine, sine):
    arrays = [a for a, _, _, _ in text] + list(image) + [a for a, _ in keyval]
    n_text, count = len(text), len(arrays)
    plan = [
        (n_text + 2 + n, *part) for n, (_, parts) in enumerate(keyval) for part in parts
    ]

    def kernel(where_ref, *refs):
        gain_ref, cos_ref, sin_ref = refs[count : count + 3]
        a_ref, key_ref, value_ref = refs[count + 3 : count + 6]
        b_ref, sem = refs[count + 6 :]
        x, z, y, c = where_ref[0], where_ref[1], where_ref[2], where_ref[3]
        start, n_rows = where_ref[4], where_ref[5]
        loads = []
        for k, (n, dx, dz, row, rows, at) in enumerate(plan):
            d = lax.rem(x + (dx + NX), NX) * NZ + lax.rem(z + (dz + NZ), NZ)
            first = pl.multiple_of(d * 256 + row, 128)
            loads.append(
                pltpu.make_async_copy(
                    refs[n].at[pl.ds(at, rows), :], b_ref.at[pl.ds(first, rows), :], sem.at[k]
                )
            )
        for copy in loads:
            copy.start()

        total = {}
        for n, (_, dy, first, flip) in enumerate(text):
            rows = refs[n].shape[0]
            side = lax.rem(y + (dy + NY), NY)
            t = side * NC + (c if flip == 0 else 1 - c)
            p_at = lax.broadcasted_iota(jnp.int32, (rows, SPAN), 0) + first - start
            j_at = lax.broadcasted_iota(jnp.int32, (rows, SPAN), 1)
            pick = jnp.where((p_at == j_at) & (j_at < n_rows), 1.0, 0.0).astype(jnp.bfloat16)
            rows_at = lax.broadcasted_iota(jnp.int32, (rows, 1), 0) + first - start
            is_image = (rows_at >= 0) & (rows_at < n_rows)
            placed = jnp.dot(
                pick, refs[n_text + flip][side], preferred_element_type=jnp.float32
            )
            value = jnp.where(is_image, placed, refs[n][...].astype(jnp.float32))
            a_ref[t, first : first + rows, :] = value.astype(jnp.bfloat16)
            squares = jnp.sum(value * value, axis=1, keepdims=True)
            if rows < SEQ:
                zero = jnp.zeros((SEQ - rows, 1), jnp.float32)
                squares = jnp.concatenate([squares, zero] if first == 0 else [zero, squares], axis=0)
            total = squares if n == 0 else total + squares
        scale = lax.rsqrt(total * (1.0 / WIDTH) + decoder_epsilon)
        for copy in loads:
            copy.wait()
        acc = jnp.zeros((SEQ, 256), jnp.float32)
        for t in range(8):
            normed = (
                a_ref[t].astype(jnp.float32) * scale * gain_ref[t : t + 1, :]
            ).astype(jnp.bfloat16)
            a_ref[t] = normed
            acc = acc + jnp.dot(
                normed, b_ref[t * 1024 : (t + 1) * 1024, :], preferred_element_type=jnp.float32
            )
        key_ref[...] = rotated(acc[:, :HEAD], cos_ref[...], sin_ref[...])
        value_ref[...] = acc[:, HEAD:].astype(jnp.bfloat16)

    return pl.pallas_call(
        kernel,
        out_shape=[
            jax.ShapeDtypeStruct((8, SEQ, 1024), jnp.bfloat16),
            jax.ShapeDtypeStruct((SEQ, HEAD), jnp.bfloat16),
            jax.ShapeDtypeStruct((SEQ, HEAD), jnp.bfloat16),
        ],
        in_specs=[SMEM] + [VMEM] * (n_text + 2) + [HBM] * len(keyval) + [VMEM] * 3,
        out_specs=[VMEM] * 3,
        scratch_shapes=[
            pltpu.VMEM((WIDTH, 256), jnp.bfloat16),
            pltpu.SemaphoreType.DMA((len(plan),)),
        ],
        compiler_params=pltpu.CompilerParams(vmem_limit_bytes=48 * 1024 * 1024),
        name="prepare",
    )(where, *arrays, gain, cosine, sine)


def attention(sequence, query_w, key, value, cosine, sine):
    def kernel(a_ref, w_hbm, key_ref, value_ref, cos_ref, sin_ref, out_ref, w_ref, sem):
        loads = [
            pltpu.make_async_copy(
                w_hbm.at[pl.ds(t * 1024, 1024), :], w_ref.at[pl.ds(t * 1024, 1024), :], sem.at[t]
            )
            for t in range(8)
        ]
        for copy in loads:
            copy.start()
        acc = jnp.zeros((SEQ, 512), jnp.float32)
        for t in range(8):
            loads[t].wait()
            acc = acc + jnp.dot(
                a_ref[t], w_ref[t * 1024 : (t + 1) * 1024, :], preferred_element_type=jnp.float32
            )
        cos, sin = cos_ref[...], sin_ref[...]
        for h in range(4):
            query = rotated(acc[:, h * HEAD : (h + 1) * HEAD], cos, sin)
            for first in range(0, SEQ, 128):
                last = first + 128
                scores = lax.dot_general(
                    query[first:last], key_ref[:last, :], (((1,), (1,)), ((), ())),
                    preferred_element_type=jnp.float32,
                ) * (HEAD ** (-0.5))
                row = lax.broadcasted_iota(jnp.int32, (128, last), 0) + first
                column = lax.broadcasted_iota(jnp.int32, (128, last), 1)
                scores = jnp.where(row >= column, scores, -1e30)
                top = jnp.max(scores, axis=1, keepdims=True)
                e = jnp.exp(scores - top)
                w = (e / jnp.sum(e, axis=1, keepdims=True)).astype(jnp.bfloat16)
                out_ref[first:last, h * HEAD : (h + 1) * HEAD] = jnp.dot(
                    w, value_ref[:last, :], preferred_element_type=jnp.float32
                ).astype(jnp.bfloat16)

    return pl.pallas_call(
        kernel,
        out_shape=jax.ShapeDtypeStruct((SEQ, 512), jnp.bfloat16),
        in_specs=[VMEM, HBM] + [VMEM] * 4,
        out_specs=VMEM,
        scratch_shapes=[
            pltpu.VMEM((WIDTH, 512), jnp.bfloat16),
            pltpu.SemaphoreType.DMA((8,)),
        ],
        compiler_params=pltpu.CompilerParams(vmem_limit_bytes=48 * 1024 * 1024),
        name="attention",
    )(sequence, query_w, key, value, cosine, sine)


def vision(vis_rows, ln_gain, ln_bias, weight):
    tokens = vis_rows.shape[0] * vis_rows.shape[1]
    whole = spread(vis_rows.reshape(tokens, 2, 400), ("y", "c")).astype(jnp.float32)
    mean = jnp.mean(whole, axis=(0, 2, 3))[None, :, None, None]
    centered = whole - mean
    variance = jnp.mean(centered * centered, axis=(0, 2, 3))[None, :, None, None]
    gain = jnp.swapaxes(ln_gain.reshape(2, 8, 400), 0, 1)[:, None]
    bias = jnp.swapaxes(ln_bias.reshape(2, 8, 400), 0, 1)[:, None]
    normed = (centered * lax.rsqrt(variance + vision_epsilon) * gain + bias).astype(jnp.bfloat16)
    acts = exchange(normed.reshape(4, 2, tokens, 2, 400), "x")
    partial = jnp.einsum(
        "sctmf,cfmo->sto", acts, weight.reshape(2, 400, 2, 1024),
        preferred_element_type=jnp.float32,
    ).astype(jnp.bfloat16)
    total = None
    for k in range(NX):
        part = lax.dynamic_index_in_dim(partial, lax.axis_index("x") ^ k, 0, keepdims=False)
        part = (part if k == 0 else flip_x(part, k)).astype(jnp.float32)
        total = part if total is None else total + part
    return total.astype(jnp.bfloat16)


def step(
    vis_rows, ln_gain, ln_bias, proj_weight, text_rows, attn_gain, w_query,
    key_value_weight, tile_counts, image_offsets,
):
    x, z = lax.axis_index("x"), lax.axis_index("z")
    y, c = lax.axis_index("y"), lax.axis_index("c")
    tile_ends = jnp.cumsum(tile_counts)
    tile_firsts = tile_ends - tile_counts
    sample_ids = jnp.arange(32, dtype=jnp.int32)

    def entry(values, index):
        return jnp.sum(jnp.where(sample_ids == index, values, 0))

    proj_all = lax.all_gather(proj_weight, "z", axis=0, tiled=True)
    query_w = lax.all_gather(w_query, ("x", "z"), axis=0, tiled=True)

    image = vision(vis_rows, ln_gain, ln_bias, proj_all).reshape(8, 8, 1024)

    along_z = ring8(key_value_weight.reshape(256, 256), "z")
    offsets, at = [], 0
    for a, dz, row in along_z:
        offsets.append((dz, row, a.shape[0], at))
        at += a.shape[0]
    keyval = []
    for a, dx, first in ring4(pack([a for a, _, _ in along_z]), "x"):
        parts = [
            (dx, dz, row, rows, at - first)
            for dz, row, rows, at in offsets
            if first <= at and at + rows <= first + a.shape[0]
        ]
        keyval.append((a, parts))

    text = []
    for a, dy, row in ring4(text_rows[0], "y"):
        text.append((a, dy, row, 0))
        text.append((shift(a, "c", 1), dy, row, 1))

    place = x * NZ + z
    tiles_here = jnp.arange(8, dtype=jnp.int32) * 32 + place
    owners = jnp.sum((tile_ends[None, :] <= tiles_here[:, None]).astype(jnp.int32), axis=1)
    slots = jnp.zeros((32, 8, 1024), jnp.bfloat16)
    for r in range(8):
        slots = jnp.where((owners[r] == sample_ids)[:, None, None], image[r][None], slots)
    received = exchange(slots, ("x", "z"))
    sources = (entry(tile_firsts, place) + jnp.arange(16, dtype=jnp.int32)) % 32
    mine = received[sources].reshape(SPAN, 1024)
    own_image = spread(mine, "y")
    other_image = shift(own_image, "c", 1)

    rows = entry(tile_counts, place) * 8
    where = jnp.stack([x, z, y, c, image_offsets[0], rows]).astype(jnp.int32)
    cosine, sine = rope_tables()
    sequence, key, value = prepare(
        where, text, (own_image, other_image), keyval, attn_gain.reshape(8, 1024), cosine, sine
    )
    return attention(sequence, query_w, key, value, cosine, sine)[None]


def solution(mesh):
    fine = Mesh(mesh.devices.reshape(NX, NZ, NY, NC), ("x", "z", "y", "c"))
    dp, tensor = ("x", "z"), ("y", "c")
    in_specs = (
        P(None, dp, None, tensor), P(), P(), P(dp, None, tensor), P(dp, None, tensor), P(),
        P(dp, tensor), P(dp, None, tensor), P(), P(dp),
    )
    return jax.shard_map(
        step, mesh=fine, in_specs=in_specs, out_specs=P(dp, None, tensor), check_vma=False
    )
```

```python
import jax
import jax.numpy as jnp
from jax import lax
from jax.experimental import pallas as pl
from jax.experimental.pallas import tpu as pltpu
from jax.sharding import Mesh, PartitionSpec as P


HEAD = 128
NX, NZ, NY, NC = 4, 8, 4, 2
SEQ = 384
SPAN = 128
WIDTH = 8192
vision_epsilon = 1e-06
decoder_epsilon = 1e-05
rope_base = 500000.0


def shift(array, axis, by):
    size = lax.axis_size(axis)
    return lax.ppermute(array, axis, [(i, (i + by) % size) for i in range(size)])


def flip_x(array, flip):
    return lax.ppermute(array, "x", [(i, i ^ flip) for i in range(NX)])


def exchange(array, axis):
    return lax.all_to_all(array, axis, 0, 0, tiled=True)


def spread(array, axis):
    size = lax.axis_size(axis)
    return exchange(jnp.broadcast_to(array[None], (size, *array.shape)), axis)


def ring4(array, axis):
    half = array.shape[0] // 2
    below = shift(array, axis, 1)
    above = shift(array, axis, -1)
    far_low = shift(below[:half], axis, 1)
    far_high = shift(above[half:], axis, -1)
    return [(array, 0, 0), (below, -1, 0), (above, 1, 0), (far_low, 2, 0), (far_high, 2, half)]


def ring8(array, axis):
    half = array.shape[0] // 2
    pieces = [(array, 0, 0)]
    below = above = array
    for step in (1, 2, 3):
        below = shift(below, axis, 1)
        above = shift(above, axis, -1)
        pieces += [(below, -step, 0), (above, step, 0)]
    pieces += [(shift(below[:half], axis, 1), 4, 0), (shift(above[half:], axis, -1), 4, half)]
    return pieces


def rope_tables():
    half = HEAD // 2
    exponents = jnp.arange(half, dtype=jnp.float32) * (2.0 / HEAD)
    frequency = rope_base ** (-exponents)
    positions = jnp.arange(SEQ, dtype=jnp.int32).astype(jnp.float32)
    angles = positions[:, None] * frequency[None, :]
    cosine, sine = jnp.cos(angles), jnp.sin(angles)
    return (
        jnp.concatenate([cosine, cosine], axis=1),
        jnp.concatenate([-sine, sine], axis=1),
    )


VMEM = pl.BlockSpec(memory_space=pltpu.VMEM)
SMEM = pl.BlockSpec(memory_space=pltpu.SMEM)
HBM = pl.BlockSpec(memory_space=pltpu.HBM)


def pack(pieces):
    rows = sum(a.shape[0] for a in pieces)

    def kernel(*refs):
        at = 0
        for ref in refs[:-1]:
            refs[-1][at : at + ref.shape[0], :] = ref[...]
            at += ref.shape[0]

    return pl.pallas_call(
        kernel,
        out_shape=jax.ShapeDtypeStruct((rows, pieces[0].shape[1]), pieces[0].dtype),
        in_specs=[VMEM] * len(pieces),
        out_specs=VMEM,
        name="pack",
    )(*pieces)


def rotated(value, cos, sin):
    return (value * cos + pltpu.roll(value, 64, 1) * sin).astype(jnp.bfloat16)


def prepare(where, text, image, keyval, gain, cosine, sine):
    arrays = [a for a, _, _, _ in text] + list(image) + [a for a, _ in keyval]
    n_text, count = len(text), len(arrays)
    plan = [
        (n_text + 2 + n, *part) for n, (_, parts) in enumerate(keyval) for part in parts
    ]

    def kernel(where_ref, *refs):
        gain_ref, cos_ref, sin_ref = refs[count : count + 3]
        a_ref, key_ref, value_ref = refs[count + 3 : count + 6]
        b_ref, sem = refs[count + 6 :]
        x, z, y, c = where_ref[0], where_ref[1], where_ref[2], where_ref[3]
        start, n_rows = where_ref[4], where_ref[5]
        loads = []
        for k, (n, dx, dz, row, rows, at) in enumerate(plan):
            d = lax.rem(x + (dx + NX), NX) * NZ + lax.rem(z + (dz + NZ), NZ)
            first = pl.multiple_of(d * 256 + row, 128)
            loads.append(
                pltpu.make_async_copy(
                    refs[n].at[pl.ds(at, rows), :], b_ref.at[pl.ds(first, rows), :], sem.at[k]
                )
            )
        for copy in loads:
            copy.start()

        total = {}
        for n, (_, dy, first, flip) in enumerate(text):
            rows = refs[n].shape[0]
            side = lax.rem(y + (dy + NY), NY)
            t = side * NC + (c if flip == 0 else 1 - c)
            p_at = lax.broadcasted_iota(jnp.int32, (rows, SPAN), 0) + first - start
            j_at = lax.broadcasted_iota(jnp.int32, (rows, SPAN), 1)
            pick = jnp.where((p_at == j_at) & (j_at < n_rows), 1.0, 0.0).astype(jnp.bfloat16)
            rows_at = lax.broadcasted_iota(jnp.int32, (rows, 1), 0) + first - start
            is_image = (rows_at >= 0) & (rows_at < n_rows)
            placed = jnp.dot(
                pick, refs[n_text + flip][side], preferred_element_type=jnp.float32
            )
            value = jnp.where(is_image, placed, refs[n][...].astype(jnp.float32))
            a_ref[t, first : first + rows, :] = value.astype(jnp.bfloat16)
            squares = jnp.sum(value * value, axis=1, keepdims=True)
            if rows < SEQ:
                zero = jnp.zeros((SEQ - rows, 1), jnp.float32)
                squares = jnp.concatenate([squares, zero] if first == 0 else [zero, squares], axis=0)
            total = squares if n == 0 else total + squares
        scale = lax.rsqrt(total * (1.0 / WIDTH) + decoder_epsilon)
        for copy in loads:
            copy.wait()
        acc = jnp.zeros((SEQ, 256), jnp.float32)
        for t in range(8):
            normed = (
                a_ref[t].astype(jnp.float32) * scale * gain_ref[t : t + 1, :]
            ).astype(jnp.bfloat16)
            a_ref[t] = normed
            acc = acc + jnp.dot(
                normed, b_ref[t * 1024 : (t + 1) * 1024, :], preferred_element_type=jnp.float32
            )
        key_ref[...] = rotated(acc[:, :HEAD], cos_ref[...], sin_ref[...])
        value_ref[...] = acc[:, HEAD:].astype(jnp.bfloat16)

    return pl.pallas_call(
        kernel,
        out_shape=[
            jax.ShapeDtypeStruct((8, SEQ, 1024), jnp.bfloat16),
            jax.ShapeDtypeStruct((SEQ, HEAD), jnp.bfloat16),
            jax.ShapeDtypeStruct((SEQ, HEAD), jnp.bfloat16),
        ],
        in_specs=[SMEM] + [VMEM] * (n_text + 2) + [HBM] * len(keyval) + [VMEM] * 3,
        out_specs=[VMEM] * 3,
        scratch_shapes=[
            pltpu.VMEM((WIDTH, 256), jnp.bfloat16),
            pltpu.SemaphoreType.DMA((len(plan),)),
        ],
        compiler_params=pltpu.CompilerParams(vmem_limit_bytes=48 * 1024 * 1024),
        name="prepare",
    )(where, *arrays, gain, cosine, sine)


def attention(sequence, query_w, key, value, cosine, sine):
    def kernel(
        a_hbm, w_hbm, key_ref, value_ref, cos_ref, sin_ref, out_ref, a_ref, w_ref, a_sem, w_sem
    ):
        loads = []
        for t in range(8):
            rows = pl.ds(t * 1024, 1024)
            loads.append(
                (
                    pltpu.make_async_copy(a_hbm.at[t], a_ref.at[t], a_sem.at[t]),
                    pltpu.make_async_copy(w_hbm.at[rows, :], w_ref.at[rows, :], w_sem.at[t]),
                )
            )
            for copy in loads[-1]:
                copy.start()
        acc = jnp.zeros((SEQ, 512), jnp.float32)
        for t in range(8):
            for copy in loads[t]:
                copy.wait()
            acc = acc + jnp.dot(
                a_ref[t], w_ref[t * 1024 : (t + 1) * 1024, :], preferred_element_type=jnp.float32
            )
        cos, sin = cos_ref[...], sin_ref[...]
        at = lax.broadcasted_iota(jnp.int32, (SEQ, SEQ), 0)
        causal = at >= lax.broadcasted_iota(jnp.int32, (SEQ, SEQ), 1)
        for h in range(4):
            query = rotated(acc[:, h * HEAD : (h + 1) * HEAD], cos, sin)
            scores = lax.dot_general(
                query, key_ref[...], (((1,), (1,)), ((), ())), preferred_element_type=jnp.float32
            ) * (HEAD ** (-0.5))
            scores = jnp.where(causal, scores, -1e30)
            top = jnp.max(scores, axis=1, keepdims=True)
            e = jnp.exp(scores - top)
            w = (e * (1.0 / jnp.sum(e, axis=1, keepdims=True))).astype(jnp.bfloat16)
            out_ref[:, h * HEAD : (h + 1) * HEAD] = jnp.dot(
                w, value_ref[...], preferred_element_type=jnp.float32
            ).astype(jnp.bfloat16)

    return pl.pallas_call(
        kernel,
        out_shape=jax.ShapeDtypeStruct((SEQ, 512), jnp.bfloat16),
        in_specs=[HBM] * 2 + [VMEM] * 4,
        out_specs=VMEM,
        scratch_shapes=[
            pltpu.VMEM((8, SEQ, 1024), jnp.bfloat16),
            pltpu.VMEM((WIDTH, 512), jnp.bfloat16),
            pltpu.SemaphoreType.DMA((8,)),
            pltpu.SemaphoreType.DMA((8,)),
        ],
        compiler_params=pltpu.CompilerParams(vmem_limit_bytes=56 * 1024 * 1024),
        name="attention",
    )(sequence, query_w, key, value, cosine, sine)


def vision(vis_rows, ln_gain, ln_bias, weight):
    tokens = vis_rows.shape[0] * vis_rows.shape[1]
    whole = spread(vis_rows.reshape(tokens, 2, 400), ("y", "c")).astype(jnp.float32)
    mean = jnp.mean(whole, axis=(0, 2, 3))[None, :, None, None]
    centered = whole - mean
    variance = jnp.mean(centered * centered, axis=(0, 2, 3))[None, :, None, None]
    gain = jnp.swapaxes(ln_gain.reshape(2, 8, 400), 0, 1)[:, None]
    bias = jnp.swapaxes(ln_bias.reshape(2, 8, 400), 0, 1)[:, None]
    normed = (centered * lax.rsqrt(variance + vision_epsilon) * gain + bias).astype(jnp.bfloat16)
    acts = exchange(normed.reshape(4, 2, tokens, 2, 400), "x")
    partial = jnp.einsum(
        "sctmf,cfmo->sto", acts, weight.reshape(2, 400, 2, 1024),
        preferred_element_type=jnp.float32,
    ).astype(jnp.bfloat16)
    total = None
    for k in range(NX):
        part = lax.dynamic_index_in_dim(partial, lax.axis_index("x") ^ k, 0, keepdims=False)
        part = (part if k == 0 else flip_x(part, k)).astype(jnp.float32)
        total = part if total is None else total + part
    return total.astype(jnp.bfloat16)


def step(
    vis_rows, ln_gain, ln_bias, proj_weight, text_rows, attn_gain, w_query,
    key_value_weight, tile_counts, image_offsets,
):
    x, z = lax.axis_index("x"), lax.axis_index("z")
    y, c = lax.axis_index("y"), lax.axis_index("c")
    tile_ends = jnp.cumsum(tile_counts)
    tile_firsts = tile_ends - tile_counts
    sample_ids = jnp.arange(32, dtype=jnp.int32)

    def entry(values, index):
        return jnp.sum(jnp.where(sample_ids == index, values, 0))

    proj_all = lax.all_gather(proj_weight, "z", axis=0, tiled=True)
    query_w = lax.all_gather(w_query, ("x", "z"), axis=0, tiled=True)

    image = vision(vis_rows, ln_gain, ln_bias, proj_all).reshape(8, 8, 1024)

    along_z = ring8(key_value_weight.reshape(256, 256), "z")
    offsets, at = [], 0
    for a, dz, row in along_z:
        offsets.append((dz, row, a.shape[0], at))
        at += a.shape[0]
    keyval = []
    for a, dx, first in ring4(pack([a for a, _, _ in along_z]), "x"):
        parts = [
            (dx, dz, row, rows, at - first)
            for dz, row, rows, at in offsets
            if first <= at and at + rows <= first + a.shape[0]
        ]
        keyval.append((a, parts))

    text = []
    for a, dy, row in ring4(text_rows[0], "y"):
        text.append((a, dy, row, 0))
        text.append((shift(a, "c", 1), dy, row, 1))

    place = x * NZ + z
    tiles_here = jnp.arange(8, dtype=jnp.int32) * 32 + place
    owners = jnp.sum((tile_ends[None, :] <= tiles_here[:, None]).astype(jnp.int32), axis=1)
    slots = jnp.zeros((32, 8, 1024), jnp.bfloat16)
    for r in range(8):
        slots = jnp.where((owners[r] == sample_ids)[:, None, None], image[r][None], slots)
    received = exchange(slots, ("x", "z"))
    sources = (entry(tile_firsts, place) + jnp.arange(16, dtype=jnp.int32)) % 32
    mine = received[sources].reshape(SPAN, 1024)
    own_image = spread(mine, "y")
    other_image = shift(own_image, "c", 1)

    rows = entry(tile_counts, place) * 8
    where = jnp.stack([x, z, y, c, image_offsets[0], rows]).astype(jnp.int32)
    cosine, sine = rope_tables()
    sequence, key, value = prepare(
        where, text, (own_image, other_image), keyval, attn_gain.reshape(8, 1024), cosine, sine
    )
    return attention(sequence, query_w, key, value, cosine, sine)[None]


def solution(mesh):
    fine = Mesh(mesh.devices.reshape(NX, NZ, NY, NC), ("x", "z", "y", "c"))
    dp, tensor = ("x", "z"), ("y", "c")
    in_specs = (
        P(None, dp, None, tensor), P(), P(), P(dp, None, tensor), P(dp, None, tensor), P(),
        P(dp, tensor), P(dp, None, tensor), P(), P(dp),
    )
    return jax.shard_map(
        step, mesh=fine, in_specs=in_specs, out_specs=P(dp, None, tensor), check_vma=False
    )
```

```python
import jax
import jax.numpy as jnp
from jax import lax
from jax.experimental import pallas as pl
from jax.experimental.pallas import tpu as pltpu
from jax.sharding import Mesh, PartitionSpec as P


HEAD = 128
NX, NZ, NY, NC = 4, 8, 4, 2
SEQ = 384
SPAN = 128
WIDTH = 8192
vision_epsilon = 1e-06
decoder_epsilon = 1e-05
rope_base = 500000.0


def shift(array, axis, by):
    size = lax.axis_size(axis)
    return lax.ppermute(array, axis, [(i, (i + by) % size) for i in range(size)])


def flip_x(array, flip):
    return lax.ppermute(array, "x", [(i, i ^ flip) for i in range(NX)])


def exchange(array, axis):
    return lax.all_to_all(array, axis, 0, 0, tiled=True)


def spread(array, axis):
    size = lax.axis_size(axis)
    return exchange(jnp.broadcast_to(array[None], (size, *array.shape)), axis)


def ring4(array, axis):
    half = array.shape[0] // 2
    below = shift(array, axis, 1)
    above = shift(array, axis, -1)
    far_low = shift(below[:half], axis, 1)
    far_high = shift(above[half:], axis, -1)
    return [(array, 0, 0), (below, -1, 0), (above, 1, 0), (far_low, 2, 0), (far_high, 2, half)]


def ring8(array, axis, half):
    pieces = [(array, 0)]
    below = above = array
    for step in (1, 2, 3):
        below = shift(below, axis, 1)
        above = shift(above, axis, -1)
        pieces += [(below, -step), (above, step)]
    far = [shift(below[:half], axis, 1), shift(above[half:], axis, -1)]
    return pieces + [(jnp.concatenate(far, axis=0), 4)]


def rope_tables():
    half = HEAD // 2
    exponents = jnp.arange(half, dtype=jnp.float32) * (2.0 / HEAD)
    frequency = rope_base ** (-exponents)
    positions = jnp.arange(SEQ, dtype=jnp.int32).astype(jnp.float32)
    angles = positions[:, None] * frequency[None, :]
    cosine, sine = jnp.cos(angles), jnp.sin(angles)
    return (
        jnp.concatenate([cosine, cosine], axis=1),
        jnp.concatenate([-sine, sine], axis=1),
    )


VMEM = pl.BlockSpec(memory_space=pltpu.VMEM)
SMEM = pl.BlockSpec(memory_space=pltpu.SMEM)
HBM = pl.BlockSpec(memory_space=pltpu.HBM)


def rotated(value, cos, sin):
    return (value * cos + pltpu.roll(value, 64, 1) * sin).astype(jnp.bfloat16)


def decoder(where, text, image, gain, weight, cosine, sine):
    arrays = [a for a, _, _, _ in text] + list(image)
    n_text, count = len(text), len(arrays)

    def kernel(where_ref, *refs):
        gain_ref, w_hbm, cos_ref, sin_ref, out_ref, a_ref, w_ref, w_sem = refs[count:]
        loads = []
        for t in range(8):
            rows = pl.ds(t * 1024, 1024)
            loads.append(pltpu.make_async_copy(w_hbm.at[rows, :], w_ref.at[rows, :], w_sem.at[t]))
            loads[-1].start()
        y, c = where_ref[0], where_ref[1]
        start, n_rows = where_ref[2], where_ref[3]
        total = None
        for n, (_, dy, first, flip) in enumerate(text):
            rows = refs[n].shape[0]
            side = lax.rem(y + (dy + NY), NY)
            t = side * NC + (c if flip == 0 else 1 - c)
            p_at = lax.broadcasted_iota(jnp.int32, (rows, SPAN), 0) + first - start
            j_at = lax.broadcasted_iota(jnp.int32, (rows, SPAN), 1)
            pick = jnp.where((p_at == j_at) & (j_at < n_rows), 1.0, 0.0).astype(jnp.bfloat16)
            rows_at = lax.broadcasted_iota(jnp.int32, (rows, 1), 0) + first - start
            is_image = (rows_at >= 0) & (rows_at < n_rows)
            placed = jnp.dot(
                pick, refs[n_text + flip][side], preferred_element_type=jnp.float32
            )
            value = jnp.where(is_image, placed, refs[n][...].astype(jnp.float32))
            a_ref[t, first : first + rows, :] = value.astype(jnp.bfloat16)
            squares = jnp.sum(value * value, axis=1, keepdims=True)
            if rows < SEQ:
                zero = jnp.zeros((SEQ - rows, 1), jnp.float32)
                squares = jnp.concatenate([squares, zero] if first == 0 else [zero, squares], axis=0)
            total = squares if total is None else total + squares
        scale = lax.rsqrt(total * (1.0 / WIDTH) + decoder_epsilon)
        acc = jnp.zeros((SEQ, 768), jnp.float32)
        for t in range(8):
            normed = (
                a_ref[t].astype(jnp.float32) * scale * gain_ref[t : t + 1, :]
            ).astype(jnp.bfloat16)
            loads[t].wait()
            acc = acc + jnp.dot(
                normed, w_ref[t * 1024 : (t + 1) * 1024, :], preferred_element_type=jnp.float32
            )
        cos, sin = cos_ref[...], sin_ref[...]
        key = rotated(acc[:, 512:640], cos, sin)
        value = acc[:, 640:].astype(jnp.bfloat16)
        at = lax.broadcasted_iota(jnp.int32, (SEQ, SEQ), 0)
        causal = at >= lax.broadcasted_iota(jnp.int32, (SEQ, SEQ), 1)
        for h in range(4):
            query = rotated(acc[:, h * HEAD : (h + 1) * HEAD], cos, sin)
            scores = lax.dot_general(
                query, key, (((1,), (1,)), ((), ())), preferred_element_type=jnp.float32
            ) * (HEAD ** (-0.5))
            scores = jnp.where(causal, scores, -1e30)
            top = jnp.max(scores, axis=1, keepdims=True)
            e = jnp.exp(scores - top)
            w = (e * (1.0 / jnp.sum(e, axis=1, keepdims=True))).astype(jnp.bfloat16)
            out_ref[:, h * HEAD : (h + 1) * HEAD] = jnp.dot(
                w, value, preferred_element_type=jnp.float32
            ).astype(jnp.bfloat16)

    return pl.pallas_call(
        kernel,
        out_shape=jax.ShapeDtypeStruct((SEQ, 512), jnp.bfloat16),
        in_specs=[SMEM] + [VMEM] * (count + 1) + [HBM] + [VMEM] * 2,
        out_specs=VMEM,
        scratch_shapes=[
            pltpu.VMEM((8, SEQ, 1024), jnp.bfloat16),
            pltpu.VMEM((WIDTH, 768), jnp.bfloat16),
            pltpu.SemaphoreType.DMA((8,)),
        ],
        compiler_params=pltpu.CompilerParams(vmem_limit_bytes=52 * 1024 * 1024),
        name="decoder",
    )(where, *arrays, gain, weight, cosine, sine)


def vision(vis_rows, ln_gain, ln_bias, proj_weight, z):
    tokens = vis_rows.shape[0] * vis_rows.shape[1]
    whole = spread(vis_rows.reshape(tokens, 2, 400), ("y", "c")).astype(jnp.float32)
    mean = jnp.mean(whole, axis=(0, 2, 3))[None, :, None, None]
    centered = whole - mean
    variance = jnp.mean(centered * centered, axis=(0, 2, 3))[None, :, None, None]
    gain = jnp.swapaxes(ln_gain.reshape(2, 8, 400), 0, 1)[:, None]
    bias = jnp.swapaxes(ln_bias.reshape(2, 8, 400), 0, 1)[:, None]
    normed = (centered * lax.rsqrt(variance + vision_epsilon) * gain + bias).astype(jnp.bfloat16)
    acts = exchange(normed.reshape(4, 2, tokens, 2, 400), "x")
    blocks = acts.reshape(4, 2, tokens, 2, 4, 100)
    blocks = jnp.transpose(blocks, (1, 4, 0, 2, 3, 5)).reshape(8, 4 * tokens, 200)
    own = jnp.swapaxes(proj_weight, 0, 1).reshape(200, 1024)
    partial = None
    for piece, dz in ring8(own, "z", 96):
        block = lax.dynamic_index_in_dim(blocks, lax.rem(z + dz + NZ, NZ), 0, keepdims=False)
        term = jnp.dot(block, piece, preferred_element_type=jnp.float32)
        partial = term if partial is None else partial + term
    partial = partial.astype(jnp.bfloat16).reshape(4, tokens, 1024)
    total = None
    for k in range(NX):
        part = lax.dynamic_index_in_dim(partial, lax.axis_index("x") ^ k, 0, keepdims=False)
        part = (part if k == 0 else flip_x(part, k)).astype(jnp.float32)
        total = part if total is None else total + part
    return total.astype(jnp.bfloat16)


def step(
    vis_rows, ln_gain, ln_bias, proj_weight, text_rows, attn_gain, w_query,
    key_value_weight, tile_counts, image_offsets,
):
    x, z = lax.axis_index("x"), lax.axis_index("z")
    y, c = lax.axis_index("y"), lax.axis_index("c")
    tile_ends = jnp.cumsum(tile_counts)
    tile_firsts = tile_ends - tile_counts
    sample_ids = jnp.arange(32, dtype=jnp.int32)

    def entry(values, index):
        return jnp.sum(jnp.where(sample_ids == index, values, 0))

    both = jnp.concatenate([w_query, key_value_weight.reshape(256, 256)], axis=1)
    both_all = lax.all_gather(both, ("x", "z"), axis=0, tiled=True)

    image = vision(vis_rows, ln_gain, ln_bias, proj_weight, z).reshape(8, 8, 1024)

    text = []
    for a, dy, row in ring4(text_rows[0], "y"):
        text.append((a, dy, row, 0))
        text.append((shift(a, "c", 1), dy, row, 1))

    place = x * NZ + z
    tiles_here = jnp.arange(8, dtype=jnp.int32) * 32 + place
    owners = jnp.sum((tile_ends[None, :] <= tiles_here[:, None]).astype(jnp.int32), axis=1)
    slots = jnp.zeros((32, 8, 1024), jnp.bfloat16)
    for r in range(8):
        slots = jnp.where((owners[r] == sample_ids)[:, None, None], image[r][None], slots)
    received = exchange(slots, ("x", "z"))
    sources = (entry(tile_firsts, place) + jnp.arange(16, dtype=jnp.int32)) % 32
    mine = received[sources].reshape(SPAN, 1024)
    own_image = spread(mine, "y")
    other_image = shift(own_image, "c", 1)

    rows = entry(tile_counts, place) * 8
    where = jnp.stack([y, c, image_offsets[0], rows]).astype(jnp.int32)
    cosine, sine = rope_tables()
    gain = attn_gain.reshape(8, 1024)
    out = decoder(where, text, (own_image, other_image), gain, both_all, cosine, sine)
    return out[None]


def solution(mesh):
    fine = Mesh(mesh.devices.reshape(NX, NZ, NY, NC), ("x", "z", "y", "c"))
    dp, tensor = ("x", "z"), ("y", "c")
    in_specs = (
        P(None, dp, None, tensor), P(), P(), P(dp, None, tensor), P(dp, None, tensor), P(),
        P(dp, tensor), P(dp, None, tensor), P(), P(dp),
    )
    return jax.shard_map(
        step, mesh=fine, in_specs=in_specs, out_specs=P(dp, None, tensor), check_vma=False
    )
```

```python
import jax
import jax.numpy as jnp
from jax import lax
from jax.experimental import pallas as pl
from jax.experimental.pallas import tpu as pltpu
from jax.sharding import Mesh, PartitionSpec as P


HEAD = 128
NX, NZ, NY, NC = 4, 8, 4, 2
SEQ = 384
SPAN = 128
WIDTH = 8192
vision_epsilon = 1e-06
decoder_epsilon = 1e-05
rope_base = 500000.0


def shift(array, axis, by):
    size = lax.axis_size(axis)
    return lax.ppermute(array, axis, [(i, (i + by) % size) for i in range(size)])


def flip_x(array, flip):
    return lax.ppermute(array, "x", [(i, i ^ flip) for i in range(NX)])


def exchange(array, axis):
    return lax.all_to_all(array, axis, 0, 0, tiled=True)


def spread(array, axis):
    size = lax.axis_size(axis)
    return exchange(jnp.broadcast_to(array[None], (size, *array.shape)), axis)


def ring4(array, axis):
    half = array.shape[0] // 2
    below = shift(array, axis, 1)
    above = shift(array, axis, -1)
    far_low = shift(below[:half], axis, 1)
    far_high = shift(above[half:], axis, -1)
    return [(array, 0, 0), (below, -1, 0), (above, 1, 0), (far_low, 2, 0), (far_high, 2, half)]


def ring8(array, axis, half):
    pieces = [(array, 0)]
    below = above = array
    for step in (1, 2, 3):
        below = shift(below, axis, 1)
        above = shift(above, axis, -1)
        pieces += [(below, -step), (above, step)]
    far = [shift(below[:half], axis, 1), shift(above[half:], axis, -1)]
    return pieces + [(jnp.concatenate(far, axis=0), 4)]


def rope_tables():
    half = HEAD // 2
    exponents = jnp.arange(half, dtype=jnp.float32) * (2.0 / HEAD)
    frequency = rope_base ** (-exponents)
    positions = jnp.arange(SEQ, dtype=jnp.int32).astype(jnp.float32)
    angles = positions[:, None] * frequency[None, :]
    cosine, sine = jnp.cos(angles), jnp.sin(angles)
    return (
        jnp.concatenate([cosine, cosine], axis=1),
        jnp.concatenate([-sine, sine], axis=1),
    )


VMEM = pl.BlockSpec(memory_space=pltpu.VMEM)
SMEM = pl.BlockSpec(memory_space=pltpu.SMEM)
HBM = pl.BlockSpec(memory_space=pltpu.HBM)


def rotated(value, cos, sin):
    return (value * cos + pltpu.roll(value, 64, 1) * sin).astype(jnp.bfloat16)


def prepare(where, text, image, gain):
    arrays = [a for a, _, _, _ in text] + list(image)
    n_text, count = len(text), len(arrays)

    def kernel(where_ref, *refs):
        gain_ref, a_ref = refs[count:]
        y, c = where_ref[0], where_ref[1]
        start, n_rows = where_ref[2], where_ref[3]
        total = None
        for n, (_, dy, first, flip) in enumerate(text):
            rows = refs[n].shape[0]
            side = lax.rem(y + (dy + NY), NY)
            t = side * NC + (c if flip == 0 else 1 - c)
            p_at = lax.broadcasted_iota(jnp.int32, (rows, SPAN), 0) + first - start
            j_at = lax.broadcasted_iota(jnp.int32, (rows, SPAN), 1)
            pick = jnp.where((p_at == j_at) & (j_at < n_rows), 1.0, 0.0).astype(jnp.bfloat16)
            rows_at = lax.broadcasted_iota(jnp.int32, (rows, 1), 0) + first - start
            is_image = (rows_at >= 0) & (rows_at < n_rows)
            placed = jnp.dot(
                pick, refs[n_text + flip][side], preferred_element_type=jnp.float32
            )
            value = jnp.where(is_image, placed, refs[n][...].astype(jnp.float32))
            a_ref[t, first : first + rows, :] = value.astype(jnp.bfloat16)
            squares = jnp.sum(value * value, axis=1, keepdims=True)
            if rows < SEQ:
                zero = jnp.zeros((SEQ - rows, 1), jnp.float32)
                squares = jnp.concatenate([squares, zero] if first == 0 else [zero, squares], axis=0)
            total = squares if total is None else total + squares
        scale = lax.rsqrt(total * (1.0 / WIDTH) + decoder_epsilon)
        for t in range(8):
            a_ref[t] = (
                a_ref[t].astype(jnp.float32) * scale * gain_ref[t : t + 1, :]
            ).astype(jnp.bfloat16)

    return pl.pallas_call(
        kernel,
        out_shape=jax.ShapeDtypeStruct((8, SEQ, 1024), jnp.bfloat16),
        in_specs=[SMEM] + [VMEM] * (count + 1),
        out_specs=VMEM,
        compiler_params=pltpu.CompilerParams(vmem_limit_bytes=48 * 1024 * 1024),
        name="prepare",
    )(where, *arrays, gain)


def attention(sequence, weight, cosine, sine):
    def kernel(
        a_hbm, w_hbm, cos_ref, sin_ref, out_ref, a_ref, w_ref, a_sem, w_sem
    ):
        loads = []
        for t in range(8):
            rows = pl.ds(t * 1024, 1024)
            loads.append(
                (
                    pltpu.make_async_copy(a_hbm.at[t], a_ref.at[t], a_sem.at[t]),
                    pltpu.make_async_copy(w_hbm.at[rows, :], w_ref.at[rows, :], w_sem.at[t]),
                )
            )
            for copy in loads[-1]:
                copy.start()
        acc = jnp.zeros((SEQ, 768), jnp.float32)
        for t in range(8):
            for copy in loads[t]:
                copy.wait()
            acc = acc + jnp.dot(
                a_ref[t], w_ref[t * 1024 : (t + 1) * 1024, :], preferred_element_type=jnp.float32
            )
        cos, sin = cos_ref[...], sin_ref[...]
        key = rotated(acc[:, 512:640], cos, sin)
        value = acc[:, 640:].astype(jnp.bfloat16)
        at = lax.broadcasted_iota(jnp.int32, (SEQ, SEQ), 0)
        causal = at >= lax.broadcasted_iota(jnp.int32, (SEQ, SEQ), 1)
        for h in range(4):
            query = rotated(acc[:, h * HEAD : (h + 1) * HEAD], cos, sin)
            scores = lax.dot_general(
                query, key, (((1,), (1,)), ((), ())), preferred_element_type=jnp.float32
            ) * (HEAD ** (-0.5))
            scores = jnp.where(causal, scores, -1e30)
            top = jnp.max(scores, axis=1, keepdims=True)
            e = jnp.exp(scores - top)
            w = (e * (1.0 / jnp.sum(e, axis=1, keepdims=True))).astype(jnp.bfloat16)
            out_ref[:, h * HEAD : (h + 1) * HEAD] = jnp.dot(
                w, value, preferred_element_type=jnp.float32
            ).astype(jnp.bfloat16)

    return pl.pallas_call(
        kernel,
        out_shape=jax.ShapeDtypeStruct((SEQ, 512), jnp.bfloat16),
        in_specs=[HBM] * 2 + [VMEM] * 2,
        out_specs=VMEM,
        scratch_shapes=[
            pltpu.VMEM((8, SEQ, 1024), jnp.bfloat16),
            pltpu.VMEM((WIDTH, 768), jnp.bfloat16),
            pltpu.SemaphoreType.DMA((8,)),
            pltpu.SemaphoreType.DMA((8,)),
        ],
        compiler_params=pltpu.CompilerParams(vmem_limit_bytes=56 * 1024 * 1024),
        name="attention",
    )(sequence, weight, cosine, sine)


def vision(vis_rows, ln_gain, ln_bias, proj_weight, z):
    tokens = vis_rows.shape[0] * vis_rows.shape[1]
    whole = spread(vis_rows.reshape(tokens, 2, 400), ("y", "c")).astype(jnp.float32)
    mean = jnp.mean(whole, axis=(0, 2, 3))[None, :, None, None]
    centered = whole - mean
    variance = jnp.mean(centered * centered, axis=(0, 2, 3))[None, :, None, None]
    gain = jnp.swapaxes(ln_gain.reshape(2, 8, 400), 0, 1)[:, None]
    bias = jnp.swapaxes(ln_bias.reshape(2, 8, 400), 0, 1)[:, None]
    normed = (centered * lax.rsqrt(variance + vision_epsilon) * gain + bias).astype(jnp.bfloat16)
    acts = exchange(normed.reshape(4, 2, tokens, 2, 400), "x")
    blocks = acts.reshape(4, 2, tokens, 2, 4, 100)
    blocks = jnp.transpose(blocks, (1, 4, 0, 2, 3, 5)).reshape(8, 4 * tokens, 200)
    own = jnp.swapaxes(proj_weight, 0, 1).reshape(200, 1024)
    partial = None
    for piece, dz in ring8(own, "z", 96):
        block = lax.dynamic_index_in_dim(blocks, lax.rem(z + dz + NZ, NZ), 0, keepdims=False)
        term = jnp.dot(block, piece, preferred_element_type=jnp.float32)
        partial = term if partial is None else partial + term
    partial = partial.astype(jnp.bfloat16).reshape(4, tokens, 1024)
    total = None
    for k in range(NX):
        part = lax.dynamic_index_in_dim(partial, lax.axis_index("x") ^ k, 0, keepdims=False)
        part = (part if k == 0 else flip_x(part, k)).astype(jnp.float32)
        total = part if total is None else total + part
    return total.astype(jnp.bfloat16)


def step(
    vis_rows, ln_gain, ln_bias, proj_weight, text_rows, attn_gain, w_query,
    key_value_weight, tile_counts, image_offsets,
):
    x, z = lax.axis_index("x"), lax.axis_index("z")
    y, c = lax.axis_index("y"), lax.axis_index("c")
    tile_ends = jnp.cumsum(tile_counts)
    tile_firsts = tile_ends - tile_counts
    sample_ids = jnp.arange(32, dtype=jnp.int32)

    def entry(values, index):
        return jnp.sum(jnp.where(sample_ids == index, values, 0))

    both = jnp.concatenate([w_query, key_value_weight.reshape(256, 256)], axis=1)
    both_all = lax.all_gather(both, ("x", "z"), axis=0, tiled=True)

    image = vision(vis_rows, ln_gain, ln_bias, proj_weight, z).reshape(8, 8, 1024)

    text = []
    for a, dy, row in ring4(text_rows[0], "y"):
        text.append((a, dy, row, 0))
        text.append((shift(a, "c", 1), dy, row, 1))

    place = x * NZ + z
    tiles_here = jnp.arange(8, dtype=jnp.int32) * 32 + place
    owners = jnp.sum((tile_ends[None, :] <= tiles_here[:, None]).astype(jnp.int32), axis=1)
    slots = jnp.zeros((32, 8, 1024), jnp.bfloat16)
    for r in range(8):
        slots = jnp.where((owners[r] == sample_ids)[:, None, None], image[r][None], slots)
    received = exchange(slots, ("x", "z"))
    sources = (entry(tile_firsts, place) + jnp.arange(16, dtype=jnp.int32)) % 32
    mine = received[sources].reshape(SPAN, 1024)
    own_image = spread(mine, "y")
    other_image = shift(own_image, "c", 1)

    rows = entry(tile_counts, place) * 8
    where = jnp.stack([y, c, image_offsets[0], rows]).astype(jnp.int32)
    cosine, sine = rope_tables()
    sequence = prepare(where, text, (own_image, other_image), attn_gain.reshape(8, 1024))
    return attention(sequence, both_all, cosine, sine)[None]


def solution(mesh):
    fine = Mesh(mesh.devices.reshape(NX, NZ, NY, NC), ("x", "z", "y", "c"))
    dp, tensor = ("x", "z"), ("y", "c")
    in_specs = (
        P(None, dp, None, tensor), P(), P(), P(dp, None, tensor), P(dp, None, tensor), P(),
        P(dp, tensor), P(dp, None, tensor), P(), P(dp),
    )
    return jax.shard_map(
        step, mesh=fine, in_specs=in_specs, out_specs=P(dp, None, tensor), check_vma=False
    )
```
